32 devices in a mesh: gx: 8 (over y, x, core), gy: 4 (over z).
Axes of the slice: x: 2, y: 2, z: 4, core: 2. Of those that a mesh axis runs over, the one named last changes fastest.
Arguments:
- east_class: int32 [512, 256], P('gx', 'gy'), may hold values from 0 to 7
- south_class: int32 [512, 256], P('gx', 'gy'), may hold values from 0 to 7
- cond_table: float32 [8], replicated, may hold values from 0.5 to 4
- leakage: float32 [512, 256], P('gx', 'gy'), may hold values from 0.1 to 1
- pad_mask: int32 [512, 256], P('gx', 'gy'), may hold values 0 or 1
- load_current: float32 [512, 256, 256], P('gx', 'gy'), may hold values from -24 to 24
Outputs:
- potential: float32 [512, 256, 256], P('gx', 'gy')
The draws below stay inside these ranges and needn't reach their ends.
All inputs are finite; a program needn't handle non-finite values. No bound on the sum of `pad_mask` on one device may be relied on, other than what follows from the above.
Results may differ from the reference program's by a relative error of at most 0.00002.
Values sent between devices are 32-bit elements; how exact they have to be, the bound alone decides.
A program may use at most 64 MiB of HBM per device.

```python
import math
import jax
import jax.numpy as jnp

CASES = 256
CLASSES = 8
ITERS = 4
NX = 512
NY = 256


def touch_ends(values, key, smallest, top_value):
    extent = values.shape
    spot = [jax.random.randint(jax.random.fold_in(key, axis), (), 0, extent[axis]) for axis in range(len(extent))]
    values = values.at[tuple(spot)].set(smallest)
    longest = extent.index(max(extent))
    spot[longest] = (spot[longest] + 1) % extent[longest]
    return values.at[tuple(spot)].set(top_value)


def shard_levels(stream_key, shape, pieces, smallest, high):
    gain, own = 1.0, jax.random.fold_in(stream_key, 6)
    for axis_at, shards_of in pieces:
        draws = jnp.exp(jax.random.uniform(jax.random.fold_in(own, axis_at), (shards_of,), jnp.float32, smallest / len(pieces), high / len(pieces)))
        gain = gain * jnp.repeat(draws, shape[axis_at] // shards_of).reshape([-1 if axis == axis_at else 1 for axis in range(len(shape))])
    return gain


def scatter_about(stream_key, dims, deviation, bound, split=(), kind=jnp.bfloat16):
    array = deviation * jax.random.normal(stream_key, dims, jnp.float32)
    if split:
        array = array * shard_levels(stream_key, dims, split, -0.22, 0.18)
    return jnp.clip(array, -bound, bound).astype(kind)


def setup_inputs(seed: int = 0) -> dict:
    streams_of = jax.random.split(jax.random.key(seed), 7)
    east_class = touch_ends(jax.random.randint(streams_of[0], (NX, NY), 0, CLASSES), jax.random.fold_in(streams_of[0], 1), 0, CLASSES - 1).astype(jnp.int32)
    south_class = touch_ends(jax.random.randint(streams_of[1], (NX, NY), 0, CLASSES), jax.random.fold_in(streams_of[1], 1), 0, CLASSES - 1).astype(jnp.int32)
    cond_table = jnp.clip(jnp.exp(jax.random.uniform(streams_of[2], (CLASSES,), jnp.float32, math.log(0.5), math.log(4.0))), 0.5, 4.0)
    leakage = jnp.clip(jnp.exp(math.log(1.0) - 2.3025851 * jax.random.uniform(streams_of[3], (NX, NY), jnp.float32) ** shard_levels(streams_of[3], (NX, NY), ((0, 8), (1, 4)), -0.2, 0.2)), 0.1, 1.0)
    pad_mask = touch_ends((jax.random.randint(streams_of[4], (NX, NY), 0, 8) < 1).astype(jnp.int32), jax.random.fold_in(streams_of[4], 1), 0, 1)
    load_current = scatter_about(streams_of[5], (NX, NY, CASES), 4.0, 24.0, ((0, 8), (1, 4)), jnp.float32)
    return dict(east_class=east_class, south_class=south_class, cond_table=cond_table, leakage=leakage, pad_mask=pad_mask, load_current=load_current)


PAD_GAIN = 8.0
SPECTRAL_BOUND = 0.995


def chebyshev_weights(total_steps):
    weights = [1.0]
    for position in range(1, total_steps):
        if position == 1:
            weights.append(1.0 / (1.0 - SPECTRAL_BOUND * SPECTRAL_BOUND / 2.0))
        else:
            weights.append(1.0 / (1.0 - SPECTRAL_BOUND * SPECTRAL_BOUND * weights[-1] / 4.0))
    return weights


def lookup(classes, cond_table):
    labels = jnp.arange(cond_table.shape[0], dtype=jnp.int32)
    matches = classes[:, :, None] == labels
    return jnp.sum(jnp.where(matches, cond_table, 0.0), axis=-1)


def reference(east_class, south_class, cond_table, leakage, pad_mask, load_current):
    east_cond = lookup(east_class, cond_table)
    south_cond = lookup(south_class, cond_table)
    pads = pad_mask.astype(jnp.float32)
    east_west = jnp.roll(east_cond, 1, 1)
    south_north = jnp.roll(south_cond, 1, 0)
    diagonal = east_cond + east_west + south_cond + south_north + (leakage + PAD_GAIN * pads)
    source = (PAD_GAIN * pads[:, :, None] - load_current) / diagonal[:, :, None]
    omegas = chebyshev_weights(ITERS)
    field = source
    previous = source
    for iteration in range(ITERS):
        neighbours = east_cond[:, :, None] * jnp.roll(field, -1, 1) + east_west[:, :, None] * jnp.roll(field, 1, 1)
        neighbours = neighbours + south_cond[:, :, None] * jnp.roll(field, -1, 0)
        neighbours = neighbours + south_north[:, :, None] * jnp.roll(field, 1, 0)
        jacobi_value = source + neighbours / diagonal[:, :, None]
        if iteration == 0:
            updated = jacobi_value
        else:
            updated = omegas[iteration] * (jacobi_value - previous) + previous
        previous, field = field, updated
    return field
```

```python
import functools

import jax
import jax.numpy as jnp
from jax import lax
from jax.experimental import pallas as pl
from jax.experimental.pallas import tpu as pltpu
from jax.sharding import PartitionSpec as P

ITERS = 4
PAD_GAIN = 8.0
SPECTRAL_BOUND = 0.995
G = ITERS
MESH = pl.DeviceIdType.MESH


def polynomial():
    weights = [1.0]
    for k in range(1, ITERS):
        if k == 1:
            weights.append(1.0 / (1.0 - SPECTRAL_BOUND**2 / 2.0))
        else:
            weights.append(1.0 / (1.0 - SPECTRAL_BOUND**2 * weights[-1] / 4.0))
    size = ITERS + 1
    previous = [1.0] + [0.0] * (size - 1)
    field = [1.0, 1.0] + [0.0] * (size - 2)
    for k in range(1, ITERS):
        jac = [1.0] + field[:-1]
        updated = [weights[k] * (a - b) + b for a, b in zip(jac, previous)]
        previous, field = field, updated
    return field


def loop(lo, count, width, compute):
    def turn(start, size):
        pending = [compute(start + u) for u in range(size)]
        for stores in pending:
            for put in stores:
                put()

    turns, rest = count // width, count % width
    if turns:
        lax.fori_loop(0, turns, lambda t, c: (turn(lo + t * width, width), c)[1], 0)
    if rest:
        turn(lo + turns * width, rest)


def setter(ref, index, value):
    def put():
        ref[index] = value
    return put


EAST, SOUTH, ROOT, PADS = range(4)


def kernel(
    nx, ny, rows, cols,
    table_hbm, east_hbm, south_hbm, leak_hbm, pad_hbm, x_ref, o_ref,
    table_ref, east_ref, south_ref, leak_ref, pad_ref,
    cf, tw, dn, load, src, v1, v2, v3, bc, eload,
    small_sem, local_sem, send_sem, recv_sem,
):
    mx, my = lax.axis_index("gx"), lax.axis_index("gy")
    north, south = lax.rem(mx + nx - 1, nx), lax.rem(mx + 1, nx)
    west, east = lax.rem(my + ny - 1, ny), lax.rem(my + 1, ny)
    cases = x_ref.shape[2]
    halves = [slice(h * 128, (h + 1) * 128) for h in range(cases // 128)]
    poly = polynomial()

    barrier = pltpu.get_barrier_semaphore()
    peers = [(north, my), (south, my), (mx, west), (mx, east)]
    for peer in peers:
        pl.semaphore_signal(barrier, inc=1, device_id=peer, device_id_type=MESH)
    small = [
        pltpu.make_async_copy(there, here, small_sem.at[n])
        for n, (there, here) in enumerate([
            (table_hbm, table_ref), (east_hbm, east_ref), (south_hbm, south_ref),
            (leak_hbm, leak_ref), (pad_hbm, pad_ref),
        ])
    ]
    for copy in small:
        copy.start()
    own = pltpu.make_async_copy(x_ref, load.at[pl.ds(G, rows)], local_sem)
    own.start()
    for copy in small:
        copy.wait()

    def lookup(classes):
        value = jnp.full(classes.shape, table_ref[0], jnp.float32)
        for c in range(1, table_ref.shape[0]):
            value = jnp.where(classes == c, table_ref[c], value)
        return value

    blank = jnp.zeros((rows, 128 - cols), jnp.float32)
    fields = [
        lookup(east_ref[...]),
        lookup(south_ref[...]),
        leak_ref[...] + PAD_GAIN * pad_ref[...].astype(jnp.float32),
    ]
    for f in range(3):
        cf[f, pl.ds(8, rows), :] = jnp.concatenate([fields[f], blank], axis=1)
    above, below = jnp.zeros((8, 128), jnp.float32), jnp.zeros((120 - rows, 128), jnp.float32)
    for f in range(3):
        square = jnp.concatenate([above, jnp.concatenate([fields[f], blank], axis=1), below], axis=0)
        tw[f, pl.ds(8, cols), :] = jnp.transpose(square)[0:cols, :]

    pl.semaphore_wait(barrier, len(peers))
    own.wait()

    counter = [0]

    def send(source, target, device):
        n = counter[0]
        counter[0] += 1
        copy = pltpu.make_async_remote_copy(
            src_ref=source, dst_ref=target,
            send_sem=send_sem.at[n], recv_sem=recv_sem.at[n],
            device_id=device, device_id_type=MESH,
        )
        copy.start()
        return copy

    def side(count, at):
        return [
            send(
                load.at[pl.ds(at, count), pl.ds(cols - G, G)],
                eload.at[0, pl.ds(at, count), pl.ds(0, G)],
                (mx, east),
            ),
            send(
                load.at[pl.ds(at, count), pl.ds(0, G)],
                eload.at[1, pl.ds(at, count), pl.ds(G, G)],
                (mx, west),
            ),
        ]

    def corner(at, row, width):
        return [
            send(
                load.at[pl.ds(at, row), pl.ds(cols - width, width)],
                eload.at[0, pl.ds(at, row), pl.ds(G - width, width)],
                (mx, east),
            ),
            send(
                load.at[pl.ds(at, row), pl.ds(0, width)],
                eload.at[1, pl.ds(at, row), pl.ds(G, width)],
                (mx, west),
            ),
        ]

    cuts = [G + rows // 2, G + rows // 2 + 3 * rows // 8]
    first = side(cuts[0] - G, G)
    cf_n = send(cf.at[:, pl.ds(rows, 8)], cf.at[:, pl.ds(0, 8)], (south, my))
    cf_s = send(cf.at[:, pl.ds(8, 8)], cf.at[:, pl.ds(rows + 8, 8)], (north, my))
    ld_n = send(load.at[pl.ds(rows, G)], load.at[pl.ds(0, G)], (south, my))
    ld_s = send(load.at[pl.ds(G, G)], load.at[pl.ds(rows + G, G)], (north, my))
    D = G - 1

    def dense(lo, size, edges):
        area = pl.ds(lo, size)
        e, s, extra = (tw[f, area, :] for f in range(3))
        e_west = tw[0, pl.ds(lo - 1, size), :] if edges and lo else pltpu.roll(e, 1, 0)
        total = e + e_west + s + pltpu.roll(s, 1, 1) + extra
        root = lax.rsqrt(total)
        pads = jnp.where(extra > PAD_GAIN / 2, PAD_GAIN, 0.0)
        dn[ROOT, area, :] = root
        dn[PADS, area, :] = pads * root
        dn[SOUTH, area, :] = s * root * pltpu.roll(root, 127, 1)

    def dense_east(lo, size):
        area = pl.ds(lo, size)
        dn[EAST, area, :] = tw[0, area, :] * dn[ROOT, area, :] * dn[ROOT, pl.ds(lo + 1, size), :]

    def spread(start, size, lo, count, width):
        def block(t):
            r = lo + t * width
            amount = 128 - (r + 8 - G)
            for f in range(4):
                value = pltpu.roll(dn[f, pl.ds(start, size), :], amount, 1)
                for u in range(width):
                    bc[f, r + u, pl.ds(start, size)] = jnp.broadcast_to(value[:, u : u + 1], (size, 128))
        lax.fori_loop(0, count // width, lambda t, c: (block(t), c)[1], 0)

    dense(8, cols, False)
    dense_east(8, cols)
    spread(8, cols, G, rows, 8)

    chain = [src, v1, v2, v3]

    def source(lo, count):
        def one(r):
            return [
                setter(src, (r, n, pl.ds(8, cols)), bc[PADS, r, pl.ds(8, cols)] - load[r, :, h] * bc[ROOT, r, pl.ds(8, cols)])
                for n, h in enumerate(halves)
            ]
        loop(lo, count, 2, one)

    def gather(r, at, size):
        coefs = [
            bc[EAST, r, pl.ds(at, size)], bc[EAST, r, pl.ds(at - 1, size)],
            bc[SOUTH, r, pl.ds(at, size)], bc[SOUTH, r - 1, pl.ds(at, size)],
        ]
        return coefs

    def update(k, r, n, at, size, coefs):
        vin = chain[k - 1]
        total = coefs[0] * vin[r, n, pl.ds(at + 1, size)]
        total += coefs[1] * vin[r, n, pl.ds(at - 1, size)]
        total += coefs[2] * vin[r + 1, n, pl.ds(at, size)]
        total += coefs[3] * vin[r - 1, n, pl.ds(at, size)]
        if k == 1:
            total = total * poly[ITERS]
        total = total + poly[ITERS - k] * src[r, n, pl.ds(at, size)]
        if k == ITERS:
            total = total * bc[ROOT, r, pl.ds(at, size)]
        return total

    def step(k, lo, count):
        def one(r):
            stores = []
            coefs = gather(r, 8, cols)
            for n, h in enumerate(halves):
                total = update(k, r, n, 8, cols, coefs)
                if k == ITERS:
                    stores.append(setter(o_ref, (r - G, slice(None), h), total))
                else:
                    stores.append(setter(chain[k], (r, n, pl.ds(8, cols)), total))
            return stores

        loop(lo, count, 2, one)

    cf_n.wait_recv()
    cf_s.wait_recv()
    for f in range(3):
        tw[f, pl.ds(8, cols), :] = jnp.transpose(cf[f])[0:cols, :]
    tw_w = send(tw.at[:, pl.ds(cols + 2, 6)], tw.at[:, pl.ds(2, 6)], (mx, east))
    tw_e = send(tw.at[:, pl.ds(8, G)], tw.at[:, pl.ds(cols + 8, G)], (mx, west))
    second = side(cuts[1] - cuts[0], cuts[0])

    source(G, rows)
    for k in range(1, ITERS):
        step(k, G + k + 1, rows - 2 * k - 1)

    ld_n.wait_recv()
    ld_s.wait_recv()
    first += corner(G - 1, 1, D) + corner(G - D, D - 1, D - 1)
    third = side(rows + G - cuts[1], cuts[1])
    third += corner(rows + G, 1, D) + corner(rows + G + 1, D - 1, D - 1)
    step(ITERS, G + ITERS + 1, rows - 2 * ITERS - 1)

    dense(8, cols, False)
    dense_east(8, cols)
    spread(8, cols, 0, G + 1, G + 1)
    spread(8, cols, rows + G - 1, G + 1, G + 1)
    source(0, G + 1)
    source(rows + G, G)
    for k in range(1, ITERS + 1):
        step(k, k, G + 1)
        step(k, rows + 2 * G - k - G, G)

    tw_w.wait_recv()
    tw_e.wait_recv()
    dense(0, 16, True)
    dense(cols, 16, True)
    dense_east(0, 15)
    dense_east(cols, 15)
    spread(0, 16, 0, rows + 2 * G, 8)
    spread(cols, 16, 0, rows + 2 * G, 8)

    lane_row = lax.broadcasted_iota(jnp.int32, (2 * G, 128), 0)
    starts = [9 - G, 8 + cols - G]
    tiles = [pl.ds(start, 2 * G) for start in starts]
    ghosts = [pl.ds(8 - G, 2 * G), tiles[1]]
    mine = [pl.ds(0, G + 1), pl.ds(cols - G, G)]
    inner = [slice(G - 1, 2 * G), slice(0, G)]

    def edge_source(lo, count):
        def one(r):
            stores = []
            for n, h in enumerate(halves):
                near = pltpu.roll(load[r, pl.ds(0, 2 * G), h], G, 0)
                far = pltpu.roll(load[r, pl.ds(cols - 2 * G, 2 * G), h], G, 0)
                for w in range(2):
                    ghost = lane_row < G if w == 0 else lane_row >= G
                    full = jnp.where(ghost, eload[w, r, :, h], far if w else near)
                    value = bc[PADS, r, ghosts[w]] - full * bc[ROOT, r, ghosts[w]]
                    stores.append(setter(src, (r, n, ghosts[w]), value))
            return stores
        loop(lo, count, 4, one)

    def edge_step(k, lo, count):
        def one(r):
            stores = []
            for w in range(2):
                coefs = gather(r, starts[w], 2 * G)
                for n, h in enumerate(halves):
                    total = update(k, r, n, starts[w], 2 * G, coefs)
                    if k < ITERS:
                        stores.append(setter(chain[k], (r, n, tiles[w]), total))
                    else:
                        stores.append(setter(o_ref, (r - G, mine[w], h), total[inner[w]]))
            return stores

        loop(lo, count, 4, one)

    bounds = [0] + cuts + [rows + 2 * G]
    for m, arrived in enumerate([first, second, third]):
        for copy in arrived:
            copy.wait_recv()
        lo, hi = bounds[m], bounds[m + 1]
        edge_source(lo, hi - lo)
        for k in range(1, ITERS + 1):
            begin = k if m == 0 else lo - k
            edge_step(k, begin, hi - k - begin)
    for copy in [cf_n, cf_s, ld_n, ld_s, tw_w, tw_e] + first + second + third:
        copy.wait_send()


def body(nx, ny, east_class, south_class, cond_table, leakage, pad_mask, load_current):
    rows, cols, cases = load_current.shape
    tall = rows + 2 * G
    f32 = jnp.float32
    halves = cases // 128
    anywhere = pl.BlockSpec(memory_space=pl.ANY)
    copies = 6 + 3 * 2 + 4 * 2
    grid = (tall, halves, cols + 16, 128)
    return pl.pallas_call(
        functools.partial(kernel, nx, ny, rows, cols),
        out_shape=pltpu.VMEM(load_current.shape, f32),
        in_specs=[anywhere] * 6,
        out_specs=pl.BlockSpec(memory_space=pltpu.VMEM),
        scratch_shapes=[
            pltpu.SMEM(cond_table.shape, f32),
            pltpu.VMEM((rows, cols), jnp.int32),
            pltpu.VMEM((rows, cols), jnp.int32),
            pltpu.VMEM((rows, cols), f32),
            pltpu.VMEM((rows, cols), jnp.int32),
            pltpu.VMEM((3, 128, 128), f32),
            pltpu.VMEM((3, cols + 16, 128), f32),
            pltpu.VMEM((4, cols + 16, 128), f32),
            pltpu.VMEM((tall, cols, cases), f32),
            pltpu.VMEM(grid, f32),
            pltpu.VMEM(grid, f32),
            pltpu.VMEM(grid, f32),
            pltpu.VMEM(grid, f32),
            pltpu.VMEM((4, tall, cols + 16, 128), f32),
            pltpu.VMEM((2, tall, 2 * G, cases), f32),
            pltpu.SemaphoreType.DMA((5,)),
            pltpu.SemaphoreType.DMA,
            pltpu.SemaphoreType.DMA((copies,)),
            pltpu.SemaphoreType.DMA((copies,)),
        ],
        compiler_params=pltpu.CompilerParams(
            collective_id=0, has_side_effects=True, vmem_limit_bytes=57 * 2**20,
        ),
    )(cond_table, east_class, south_class, leakage, pad_mask, load_current)


def solution(mesh):
    in_specs = (
        P("gx", "gy"),
        P("gx", "gy"),
        P(),
        P("gx", "gy"),
        P("gx", "gy"),
        P("gx", "gy", None),
    )
    out_specs = P("gx", "gy", None)
    call = functools.partial(body, mesh.shape["gx"], mesh.shape["gy"])
    return jax.shard_map(call, mesh=mesh, in_specs=in_specs, out_specs=out_specs, check_vma=False)
```

```python
import functools

import jax
import jax.numpy as jnp
from jax import lax
from jax.experimental import pallas as pl
from jax.experimental.pallas import tpu as pltpu
from jax.sharding import PartitionSpec as P

ITERS = 4
PAD_GAIN = 8.0
SPECTRAL_BOUND = 0.995
G = ITERS
MESH = pl.DeviceIdType.MESH


def polynomial():
    weights = [1.0]
    for k in range(1, ITERS):
        if k == 1:
            weights.append(1.0 / (1.0 - SPECTRAL_BOUND**2 / 2.0))
        else:
            weights.append(1.0 / (1.0 - SPECTRAL_BOUND**2 * weights[-1] / 4.0))
    size = ITERS + 1
    previous = [1.0] + [0.0] * (size - 1)
    field = [1.0, 1.0] + [0.0] * (size - 2)
    for k in range(1, ITERS):
        jac = [1.0] + field[:-1]
        updated = [weights[k] * (a - b) + b for a, b in zip(jac, previous)]
        previous, field = field, updated
    return field


def loop(lo, count, width, compute):
    def turn(start, size):
        pending = [compute(start + u) for u in range(size)]
        for stores in pending:
            for put in stores:
                put()

    turns, rest = count // width, count % width
    if turns:
        lax.fori_loop(0, turns, lambda t, c: (turn(lo + t * width, width), c)[1], 0)
    if rest:
        turn(lo + turns * width, rest)


def setter(ref, index, value):
    def put():
        ref[index] = value
    return put


EAST, SOUTH, ROOT, PADS = range(4)


def kernel(
    nx, ny, rows, cols,
    table_hbm, east_hbm, south_hbm, leak_hbm, pad_hbm, x_ref, o_ref,
    table_ref, east_ref, south_ref, leak_ref, pad_ref,
    cf, tw, pk, pe, load, src, v1, v2, v3, bc, eload,
    small_sem, local_sem, send_sem, recv_sem,
):
    mx, my = lax.axis_index("gx"), lax.axis_index("gy")
    north, south = lax.rem(mx + nx - 1, nx), lax.rem(mx + 1, nx)
    west, east = lax.rem(my + ny - 1, ny), lax.rem(my + 1, ny)
    cases = x_ref.shape[2]
    halves = [slice(h * 128, (h + 1) * 128) for h in range(cases // 128)]
    poly = polynomial()

    barrier = pltpu.get_barrier_semaphore()
    peers = [(north, my), (south, my), (mx, west), (mx, east)]
    for peer in peers:
        pl.semaphore_signal(barrier, inc=1, device_id=peer, device_id_type=MESH)
    small = [
        pltpu.make_async_copy(there, here, small_sem.at[n])
        for n, (there, here) in enumerate([
            (table_hbm, table_ref), (east_hbm, east_ref), (south_hbm, south_ref),
            (leak_hbm, leak_ref), (pad_hbm, pad_ref),
        ])
    ]
    for copy in small:
        copy.start()
    own = pltpu.make_async_copy(x_ref, load.at[pl.ds(G, rows)], local_sem)
    own.start()
    for copy in small:
        copy.wait()

    def lookup(classes):
        value = jnp.full(classes.shape, table_ref[0], jnp.float32)
        for c in range(1, table_ref.shape[0]):
            value = jnp.where(classes == c, table_ref[c], value)
        return value

    blank = jnp.zeros((rows, 128 - cols), jnp.float32)
    fields = [
        lookup(east_ref[...]),
        lookup(south_ref[...]),
        leak_ref[...] + PAD_GAIN * pad_ref[...].astype(jnp.float32),
    ]
    for f in range(3):
        cf[f, pl.ds(8, rows), :] = jnp.concatenate([fields[f], blank], axis=1)

    pl.semaphore_wait(barrier, len(peers))
    own.wait()

    counter = [0]

    def send(source, target, device):
        n = counter[0]
        counter[0] += 1
        copy = pltpu.make_async_remote_copy(
            src_ref=source, dst_ref=target,
            send_sem=send_sem.at[n], recv_sem=recv_sem.at[n],
            device_id=device, device_id_type=MESH,
        )
        copy.start()
        return copy

    def side(count, at):
        return [
            send(
                load.at[pl.ds(at, count), pl.ds(cols - G, G)],
                eload.at[0, pl.ds(at, count), pl.ds(0, G)],
                (mx, east),
            ),
            send(
                load.at[pl.ds(at, count), pl.ds(0, G)],
                eload.at[1, pl.ds(at, count), pl.ds(G, G)],
                (mx, west),
            ),
        ]

    def corner(at, row, width):
        return [
            send(
                load.at[pl.ds(at, row), pl.ds(cols - width, width)],
                eload.at[0, pl.ds(at, row), pl.ds(G - width, width)],
                (mx, east),
            ),
            send(
                load.at[pl.ds(at, row), pl.ds(0, width)],
                eload.at[1, pl.ds(at, row), pl.ds(G, width)],
                (mx, west),
            ),
        ]

    cuts = [G + rows // 2, G + rows // 2 + 3 * rows // 8]
    first = side(cuts[0] - G, G)
    cf_n = send(cf.at[:, pl.ds(rows, 8)], cf.at[:, pl.ds(0, 8)], (south, my))
    cf_s = send(cf.at[:, pl.ds(8, 8)], cf.at[:, pl.ds(rows + 8, 8)], (north, my))
    ld_n = send(load.at[pl.ds(rows, G)], load.at[pl.ds(0, G)], (south, my))
    ld_s = send(load.at[pl.ds(G, G)], load.at[pl.ds(rows + G, G)], (north, my))
    D = G - 1

    lane = lax.broadcasted_iota(jnp.int32, (8, 128), 1)

    def dense(lo, size):
        area = pl.ds(lo, size)
        e, s, extra = (cf[f, area, :] for f in range(3))
        root = lax.rsqrt(e + pltpu.roll(e, 1, 1) + s + pltpu.roll(s, 1, 0) + extra)
        pads = jnp.where(extra > PAD_GAIN / 2, PAD_GAIN, 0.0)
        left = jnp.broadcast_to(lane[0:1] < cols, (size, 128))
        values = [e * root * pltpu.roll(root, 127, 1), s * root * pltpu.roll(root, size - 1, 0), root, pads * root]
        for p in range(2):
            pk[p, area, :] = jnp.where(left, values[2 * p], pltpu.roll(values[2 * p + 1], cols, 1))

    def dense_edge(lo):
        area = pl.ds(lo, 16)
        e, s, extra = (tw[f, area, :] for f in range(3))
        e_west = tw[0, pl.ds(lo - 1, 16), :] if lo else pltpu.roll(e, 1, 0)
        root = lax.rsqrt(e + e_west + s + pltpu.roll(s, 1, 1) + extra)
        pads = jnp.where(extra > PAD_GAIN / 2, PAD_GAIN, 0.0)
        return [e * root * pltpu.roll(root, 15, 0), s * root * pltpu.roll(root, 127, 1), root, pads * root]

    def turned(ref, r):
        return jnp.transpose(jnp.broadcast_to(ref[pl.ds(r + 8 - G, 1), :], (128, 128)))

    def spread(lo, count, width):
        def block(t):
            for u in range(width):
                r = lo + t * width + u
                for p in range(2):
                    value = turned(pk.at[p], r)
                    bc[2 * p, r, pl.ds(8, cols)] = value[0:cols]
                    bc[2 * p + 1, r, pl.ds(8, cols)] = value[cols : 2 * cols]
        lax.fori_loop(0, count // width, lambda t, c: (block(t), c)[1], 0)

    def spread_edge(lo, count, width):
        def block(t):
            for u in range(width):
                r = lo + t * width + u
                value = turned(pe, r)
                for f in range(4):
                    bc[f, r, pl.ds(0, 16)] = value[32 * f : 32 * f + 16]
                    bc[f, r, pl.ds(cols, 16)] = value[32 * f + 16 : 32 * f + 32]
        lax.fori_loop(0, count // width, lambda t, c: (block(t), c)[1], 0)

    dense(8, rows)
    spread(G, rows, 8)

    chain = [src, v1, v2, v3]

    def source(lo, count):
        def one(r):
            return [
                setter(src, (r, n, pl.ds(8, cols)), bc[PADS, r, pl.ds(8, cols)] - load[r, :, h] * bc[ROOT, r, pl.ds(8, cols)])
                for n, h in enumerate(halves)
            ]
        loop(lo, count, 2, one)

    def gather(r, at, size):
        coefs = [
            bc[EAST, r, pl.ds(at, size)], bc[EAST, r, pl.ds(at - 1, size)],
            bc[SOUTH, r, pl.ds(at, size)], bc[SOUTH, r - 1, pl.ds(at, size)],
        ]
        return coefs

    def update(k, r, n, at, size, coefs):
        vin = chain[k - 1]
        total = coefs[0] * vin[r, n, pl.ds(at + 1, size)]
        total += coefs[1] * vin[r, n, pl.ds(at - 1, size)]
        total += coefs[2] * vin[r + 1, n, pl.ds(at, size)]
        total += coefs[3] * vin[r - 1, n, pl.ds(at, size)]
        if k == 1:
            total = total * poly[ITERS]
        total = total + poly[ITERS - k] * src[r, n, pl.ds(at, size)]
        if k == ITERS:
            total = total * bc[ROOT, r, pl.ds(at, size)]
        return total

    def step(k, lo, count):
        def one(r):
            stores = []
            coefs = gather(r, 8, cols)
            for n, h in enumerate(halves):
                total = update(k, r, n, 8, cols, coefs)
                if k == ITERS:
                    stores.append(setter(o_ref, (r - G, slice(None), h), total))
                else:
                    stores.append(setter(chain[k], (r, n, pl.ds(8, cols)), total))
            return stores

        loop(lo, count, 2, one)

    cf_n.wait_recv()
    cf_s.wait_recv()
    for f in range(3):
        tw[f, pl.ds(8, cols), :] = jnp.transpose(cf[f])[0:cols, :]
    tw_w = send(tw.at[:, pl.ds(cols + 2, 6)], tw.at[:, pl.ds(2, 6)], (mx, east))
    tw_e = send(tw.at[:, pl.ds(8, G)], tw.at[:, pl.ds(cols + 8, G)], (mx, west))
    second = side(cuts[1] - cuts[0], cuts[0])

    source(G, rows)
    for k in range(1, ITERS):
        step(k, G + k + 1, rows - 2 * k - 1)

    ld_n.wait_recv()
    ld_s.wait_recv()
    first += corner(G - 1, 1, D) + corner(G - D, D - 1, D - 1)
    third = side(rows + G - cuts[1], cuts[1])
    third += corner(rows + G, 1, D) + corner(rows + G + 1, D - 1, D - 1)
    step(ITERS, G + ITERS + 1, rows - 2 * ITERS - 1)

    dense(0, rows + 16)
    spread(0, G + 1, G + 1)
    spread(rows + G - 1, G + 1, G + 1)
    source(0, G + 1)
    source(rows + G, G)
    for k in range(1, ITERS + 1):
        step(k, k, G + 1)
        step(k, rows + 2 * G - k - G, G)

    tw_w.wait_recv()
    tw_e.wait_recv()
    sides = zip(dense_edge(0), dense_edge(cols))
    pe[...] = jnp.transpose(jnp.concatenate([part for pair in sides for part in pair], axis=0))
    spread_edge(0, rows + 2 * G, 8)

    lane_row = lax.broadcasted_iota(jnp.int32, (2 * G, 128), 0)
    starts = [9 - G, 8 + cols - G]
    tiles = [pl.ds(start, 2 * G) for start in starts]
    ghosts = [pl.ds(8 - G, 2 * G), tiles[1]]
    mine = [pl.ds(0, G + 1), pl.ds(cols - G, G)]
    inner = [slice(G - 1, 2 * G), slice(0, G)]

    def edge_source(lo, count):
        def one(r):
            stores = []
            for n, h in enumerate(halves):
                near = pltpu.roll(load[r, pl.ds(0, 2 * G), h], G, 0)
                far = pltpu.roll(load[r, pl.ds(cols - 2 * G, 2 * G), h], G, 0)
                for w in range(2):
                    ghost = lane_row < G if w == 0 else lane_row >= G
                    full = jnp.where(ghost, eload[w, r, :, h], far if w else near)
                    value = bc[PADS, r, ghosts[w]] - full * bc[ROOT, r, ghosts[w]]
                    stores.append(setter(src, (r, n, ghosts[w]), value))
            return stores
        loop(lo, count, 4, one)

    def edge_step(k, lo, count):
        def one(r):
            stores = []
            for w in range(2):
                coefs = gather(r, starts[w], 2 * G)
                for n, h in enumerate(halves):
                    total = update(k, r, n, starts[w], 2 * G, coefs)
                    if k < ITERS:
                        stores.append(setter(chain[k], (r, n, tiles[w]), total))
                    else:
                        stores.append(setter(o_ref, (r - G, mine[w], h), total[inner[w]]))
            return stores

        loop(lo, count, 4, one)

    bounds = [0] + cuts + [rows + 2 * G]
    for m, arrived in enumerate([first, second, third]):
        for copy in arrived:
            copy.wait_recv()
        lo, hi = bounds[m], bounds[m + 1]
        edge_source(lo, hi - lo)
        for k in range(1, ITERS + 1):
            begin = k if m == 0 else lo - k
            edge_step(k, begin, hi - k - begin)
    for copy in [cf_n, cf_s, ld_n, ld_s, tw_w, tw_e] + first + second + third:
        copy.wait_send()


def body(nx, ny, east_class, south_class, cond_table, leakage, pad_mask, load_current):
    rows, cols, cases = load_current.shape
    tall = rows + 2 * G
    f32 = jnp.float32
    halves = cases // 128
    anywhere = pl.BlockSpec(memory_space=pl.ANY)
    copies = 6 + 3 * 2 + 4 * 2
    grid = (tall, halves, cols + 16, 128)
    return pl.pallas_call(
        functools.partial(kernel, nx, ny, rows, cols),
        out_shape=pltpu.VMEM(load_current.shape, f32),
        in_specs=[anywhere] * 6,
        out_specs=pl.BlockSpec(memory_space=pltpu.VMEM),
        scratch_shapes=[
            pltpu.SMEM(cond_table.shape, f32),
            pltpu.VMEM((rows, cols), jnp.int32),
            pltpu.VMEM((rows, cols), jnp.int32),
            pltpu.VMEM((rows, cols), f32),
            pltpu.VMEM((rows, cols), jnp.int32),
            pltpu.VMEM((3, 128, 128), f32),
            pltpu.VMEM((3, cols + 16, 128), f32),
            pltpu.VMEM((2, 128, 128), f32),
            pltpu.VMEM((128, 128), f32),
            pltpu.VMEM((tall, cols, cases), f32),
            pltpu.VMEM(grid, f32),
            pltpu.VMEM(grid, f32),
            pltpu.VMEM(grid, f32),
            pltpu.VMEM(grid, f32),
            pltpu.VMEM((4, tall, cols + 16, 128), f32),
            pltpu.VMEM((2, tall, 2 * G, cases), f32),
            pltpu.SemaphoreType.DMA((5,)),
            pltpu.SemaphoreType.DMA,
            pltpu.SemaphoreType.DMA((copies,)),
            pltpu.SemaphoreType.DMA((copies,)),
        ],
        compiler_params=pltpu.CompilerParams(
            collective_id=0, has_side_effects=True, vmem_limit_bytes=57 * 2**20,
        ),
    )(cond_table, east_class, south_class, leakage, pad_mask, load_current)


def solution(mesh):
    in_specs = (
        P("gx", "gy"),
        P("gx", "gy"),
        P(),
        P("gx", "gy"),
        P("gx", "gy"),
        P("gx", "gy", None),
    )
    out_specs = P("gx", "gy", None)
    call = functools.partial(body, mesh.shape["gx"], mesh.shape["gy"])
    return jax.shard_map(call, mesh=mesh, in_specs=in_specs, out_specs=out_specs, check_vma=False)
```

```python
import functools

import jax
import jax.numpy as jnp
from jax import lax
from jax.experimental import pallas as pl
from jax.experimental.pallas import tpu as pltpu
from jax.sharding import PartitionSpec as P

ITERS = 4
PAD_GAIN = 8.0
SPECTRAL_BOUND = 0.995
G = ITERS
MESH = pl.DeviceIdType.MESH


def polynomial():
    weights = [1.0]
    for k in range(1, ITERS):
        if k == 1:
            weights.append(1.0 / (1.0 - SPECTRAL_BOUND**2 / 2.0))
        else:
            weights.append(1.0 / (1.0 - SPECTRAL_BOUND**2 * weights[-1] / 4.0))
    size = ITERS + 1
    previous = [1.0] + [0.0] * (size - 1)
    field = [1.0, 1.0] + [0.0] * (size - 2)
    for k in range(1, ITERS):
        jac = [1.0] + field[:-1]
        updated = [weights[k] * (a - b) + b for a, b in zip(jac, previous)]
        previous, field = field, updated
    return field


def loop(lo, count, width, compute):
    def turn(start, size):
        pending = [compute(start + u) for u in range(size)]
        for stores in pending:
            for put in stores:
                put()

    turns, rest = count // width, count % width
    if turns:
        lax.fori_loop(0, turns, lambda t, c: (turn(lo + t * width, width), c)[1], 0)
    if rest:
        turn(lo + turns * width, rest)


def setter(ref, index, value):
    def put():
        ref[index] = value
    return put


EAST, SOUTH, ROOT, PADS = range(4)


def kernel(
    nx, ny, rows, cols,
    table_hbm, east_hbm, south_hbm, leak_hbm, pad_hbm, x_ref, o_ref,
    table_ref, east_ref, south_ref, leak_ref, pad_ref,
    cf, tw, pk, pe, load, src, v1, v2, v3, bc, eload,
    small_sem, rim_sem, local_sem, send_sem, recv_sem,
):
    mx, my = lax.axis_index("gx"), lax.axis_index("gy")
    north, south = lax.rem(mx + nx - 1, nx), lax.rem(mx + 1, nx)
    west, east = lax.rem(my + ny - 1, ny), lax.rem(my + 1, ny)
    cases = x_ref.shape[2]
    halves = [slice(h * 128, (h + 1) * 128) for h in range(cases // 128)]
    poly = polynomial()

    barrier = pltpu.get_barrier_semaphore()
    peers = [(north, my), (south, my), (mx, west), (mx, east)]
    for peer in peers:
        pl.semaphore_signal(barrier, inc=1, device_id=peer, device_id_type=MESH)
    small = [
        pltpu.make_async_copy(there, here, small_sem.at[n])
        for n, (there, here) in enumerate([
            (table_hbm, table_ref), (east_hbm, east_ref), (south_hbm, south_ref),
            (leak_hbm, leak_ref), (pad_hbm, pad_ref),
        ])
    ]
    for copy in small:
        copy.start()
    area = pl.ds(G, rows)
    rims = [
        pltpu.make_async_copy(x_ref.at[:, pl.ds(0, G)], eload.at[0, area, pl.ds(G, G)], rim_sem.at[0]),
        pltpu.make_async_copy(x_ref.at[:, pl.ds(cols - G, G)], eload.at[1, area, pl.ds(0, G)], rim_sem.at[1]),
    ]
    for copy in rims:
        copy.start()
    own = pltpu.make_async_copy(x_ref, load.at[area], local_sem)
    own.start()
    for copy in small:
        copy.wait()

    def lookup(classes):
        value = jnp.full(classes.shape, table_ref[0], jnp.float32)
        for c in range(1, table_ref.shape[0]):
            value = jnp.where(classes == c, table_ref[c], value)
        return value

    blank = jnp.zeros((rows, 128 - cols), jnp.float32)
    fields = [
        lookup(east_ref[...]),
        lookup(south_ref[...]),
        leak_ref[...] + PAD_GAIN * pad_ref[...].astype(jnp.float32),
    ]
    for f in range(3):
        cf[f, pl.ds(8, rows), :] = jnp.concatenate([fields[f], blank], axis=1)

    pl.semaphore_wait(barrier, len(peers))
    for copy in rims:
        copy.wait()

    counter = [0]

    def send(source, target, device):
        n = counter[0]
        counter[0] += 1
        copy = pltpu.make_async_remote_copy(
            src_ref=source, dst_ref=target,
            send_sem=send_sem.at[n], recv_sem=recv_sem.at[n],
            device_id=device, device_id_type=MESH,
        )
        copy.start()
        return copy

    def side(at, count):
        return [
            send(
                eload.at[1, pl.ds(at, count), pl.ds(0, G)],
                eload.at[0, pl.ds(at, count), pl.ds(0, G)],
                (mx, east),
            ),
            send(
                eload.at[0, pl.ds(at, count), pl.ds(G, G)],
                eload.at[1, pl.ds(at, count), pl.ds(G, G)],
                (mx, west),
            ),
        ]

    cuts = [G + rows // 2, G + rows // 2 + 5 * rows // 16]
    ends = side(G, G) + side(rows, G)
    first = side(2 * G, cuts[0] - 2 * G)
    cf_n = send(cf.at[:, pl.ds(rows, 8)], cf.at[:, pl.ds(0, 8)], (south, my))
    cf_s = send(cf.at[:, pl.ds(8, 8)], cf.at[:, pl.ds(rows + 8, 8)], (north, my))
    ld_n = send(x_ref.at[pl.ds(rows - G, G)], load.at[pl.ds(0, G)], (south, my))
    ld_s = send(x_ref.at[pl.ds(0, G)], load.at[pl.ds(rows + G, G)], (north, my))

    lane = lax.broadcasted_iota(jnp.int32, (8, 128), 1)

    def dense(lo, size):
        area = pl.ds(lo, size)
        e, s, extra = (cf[f, area, :] for f in range(3))
        root = lax.rsqrt(e + pltpu.roll(e, 1, 1) + s + pltpu.roll(s, 1, 0) + extra)
        pads = jnp.where(extra > PAD_GAIN / 2, PAD_GAIN, 0.0)
        left = jnp.broadcast_to(lane[0:1] < cols, (size, 128))
        values = [e * root * pltpu.roll(root, 127, 1), s * root * pltpu.roll(root, size - 1, 0), root, pads * root]
        for p in range(2):
            pk[p, area, :] = jnp.where(left, values[2 * p], pltpu.roll(values[2 * p + 1], cols, 1))

    def dense_edge(lo):
        size = 16 if lo else 24
        area = pl.ds(lo, size)
        e, s, extra = (tw[f, area, :] for f in range(3))
        e_west = tw[0, pl.ds(lo - 1, size), :] if lo else pltpu.roll(e, 1, 0)
        root = lax.rsqrt(e + e_west + s + pltpu.roll(s, 1, 1) + extra)
        pads = jnp.where(extra > PAD_GAIN / 2, PAD_GAIN, 0.0)
        values = [e * root * pltpu.roll(root, size - 1, 0), s * root * pltpu.roll(root, 127, 1), root, pads * root]
        return [value[0:16] for value in values]

    def turned(ref, r):
        return jnp.transpose(jnp.broadcast_to(ref[pl.ds(r + 8 - G, 1), :], (128, 128)))

    def spread(lo, count, width):
        inside = pl.ds(8, cols)

        def block(t):
            for u in range(width):
                r = lo + t * width + u
                value = turned(pk.at[0], r)
                bc[EAST, r, inside] = value[0:cols]
                bc[SOUTH, r, inside] = value[cols : 2 * cols]
                value = turned(pk.at[1], r)
                bc[ROOT, r, inside] = value[0:cols]
                for n, h in enumerate(halves):
                    src[r, n, inside] = value[cols : 2 * cols] - load[r, :, h] * value[0:cols]
        lax.fori_loop(0, count // width, lambda t, c: (block(t), c)[1], 0)

    def spread_edge(lo, count, width):
        def block(t):
            for u in range(width):
                r = lo + t * width + u
                value = turned(pe, r)
                for f in range(4):
                    bc[f, r, pl.ds(0, 16)] = value[32 * f : 32 * f + 16]
                    bc[f, r, pl.ds(cols, 16)] = value[32 * f + 16 : 32 * f + 32]
        lax.fori_loop(0, count // width, lambda t, c: (block(t), c)[1], 0)

    dense(8, rows)
    own.wait()
    spread(G, rows, 8)

    chain = [src, v1, v2, v3]

    def gather(r, at, size):
        coefs = [
            bc[EAST, r, pl.ds(at, size)], bc[EAST, r, pl.ds(at - 1, size)],
            bc[SOUTH, r, pl.ds(at, size)], bc[SOUTH, r - 1, pl.ds(at, size)],
        ]
        return coefs

    def update(k, r, n, at, size, coefs):
        vin = chain[k - 1]
        total = coefs[0] * vin[r, n, pl.ds(at + 1, size)]
        total += coefs[1] * vin[r, n, pl.ds(at - 1, size)]
        total += coefs[2] * vin[r + 1, n, pl.ds(at, size)]
        total += coefs[3] * vin[r - 1, n, pl.ds(at, size)]
        if k == 1:
            total = total * poly[ITERS]
        total = total + poly[ITERS - k] * src[r, n, pl.ds(at, size)]
        if k == ITERS:
            total = total * bc[ROOT, r, pl.ds(at, size)]
        return total

    def step(k, lo, count):
        skip = 2 * G if k == ITERS else G
        at, size = 8 + skip, cols - 2 * skip

        def one(r):
            stores = []
            coefs = gather(r, at, size)
            for n, h in enumerate(halves):
                total = update(k, r, n, at, size, coefs)
                if k == ITERS:
                    stores.append(setter(o_ref, (r - G, pl.ds(skip, size), h), total))
                else:
                    stores.append(setter(chain[k], (r, n, pl.ds(at, size)), total))
            return stores

        loop(lo, count, 2, one)

    cf_n.wait_recv()
    cf_s.wait_recv()
    for f in range(3):
        tw[f, pl.ds(8, cols), :] = jnp.transpose(cf[f])[0:cols, :]
    tw_w = send(tw.at[:, pl.ds(cols + 2, 6)], tw.at[:, pl.ds(2, 6)], (mx, east))
    tw_e = send(tw.at[:, pl.ds(8, G)], tw.at[:, pl.ds(cols + 8, G)], (mx, west))
    second = side(cuts[0], cuts[1] - cuts[0])
    third = side(cuts[1], rows - cuts[1])

    step(1, G + 2, rows - 3)
    for copy in ends:
        copy.wait_recv()
    for w in range(2):
        first.append(send(eload.at[w, pl.ds(rows, G)], eload.at[w, pl.ds(0, G)], (south, my)))
        third.append(send(eload.at[w, pl.ds(G, G)], eload.at[w, pl.ds(rows + G, G)], (north, my)))
    for k in range(2, ITERS + 1):
        step(k, G + k + 1, rows - 2 * k - 1)

    ld_n.wait_recv()
    ld_s.wait_recv()
    dense(0, rows + 16)
    spread(0, G + 1, G + 1)
    spread(rows + G - 1, G + 1, G + 1)
    for k in range(1, ITERS + 1):
        step(k, k, G + 1)
        step(k, rows + 2 * G - k - G, G)

    tw_w.wait_recv()
    tw_e.wait_recv()
    sides = zip(dense_edge(0), dense_edge(cols))
    pe[...] = jnp.transpose(jnp.concatenate([part for pair in sides for part in pair], axis=0))
    spread_edge(0, rows + 2 * G, 8)

    edge = 2 * G
    rims_at = [[8 - G, 9 - G, 9 - G, 10 - G, 8], [8 + cols - G, 7 + cols - G, 7 + cols - G, 6 + cols - G, 8 + cols - 2 * G]]

    def edge_source(lo, count):
        def one(r):
            stores = []
            for w in range(2):
                area = pl.ds(rims_at[w][0], edge)
                pads, root = bc[PADS, r, area], bc[ROOT, r, area]
                for n, h in enumerate(halves):
                    stores.append(setter(src, (r, n, area), pads - eload[w, r, :, h] * root))
            return stores
        loop(lo, count, 4, one)

    def edge_step(k, lo, count):
        def one(r):
            stores = []
            for w in range(2):
                at = rims_at[w][k]
                coefs = gather(r, at, edge)
                for n, h in enumerate(halves):
                    total = update(k, r, n, at, edge, coefs)
                    if k < ITERS:
                        stores.append(setter(chain[k], (r, n, pl.ds(at, edge)), total))
                    else:
                        stores.append(setter(o_ref, (r - G, pl.ds(at - 8, edge), h), total))
            return stores

        loop(lo, count, 4, one)

    bounds = [0] + cuts + [rows + 2 * G]
    for m, arrived in enumerate([first, second, third]):
        for copy in arrived:
            copy.wait_recv()
        lo, hi = bounds[m], bounds[m + 1]
        edge_source(lo, hi - lo)
        for k in range(1, ITERS + 1):
            begin = k if m == 0 else lo - k
            edge_step(k, begin, hi - k - begin)
    for copy in [cf_n, cf_s, ld_n, ld_s, tw_w, tw_e] + ends + first + second + third:
        copy.wait_send()


def body(nx, ny, east_class, south_class, cond_table, leakage, pad_mask, load_current):
    rows, cols, cases = load_current.shape
    tall = rows + 2 * G
    f32 = jnp.float32
    halves = cases // 128
    anywhere = pl.BlockSpec(memory_space=pl.ANY)
    copies = 6 + 5 * 2 + 2 * 2
    grid = (tall, halves, cols + 16, 128)
    return pl.pallas_call(
        functools.partial(kernel, nx, ny, rows, cols),
        out_shape=pltpu.VMEM(load_current.shape, f32),
        in_specs=[anywhere] * 6,
        out_specs=pl.BlockSpec(memory_space=pltpu.VMEM),
        scratch_shapes=[
            pltpu.SMEM(cond_table.shape, f32),
            pltpu.VMEM((rows, cols), jnp.int32),
            pltpu.VMEM((rows, cols), jnp.int32),
            pltpu.VMEM((rows, cols), f32),
            pltpu.VMEM((rows, cols), jnp.int32),
            pltpu.VMEM((3, 128, 128), f32),
            pltpu.VMEM((3, cols + 16, 128), f32),
            pltpu.VMEM((2, 128, 128), f32),
            pltpu.VMEM((128, 128), f32),
            pltpu.VMEM((tall, cols, cases), f32),
            pltpu.VMEM(grid, f32),
            pltpu.VMEM(grid, f32),
            pltpu.VMEM(grid, f32),
            pltpu.VMEM(grid, f32),
            pltpu.VMEM((4, tall, cols + 16, 128), f32),
            pltpu.VMEM((2, tall, 2 * G, cases), f32),
            pltpu.SemaphoreType.DMA((5,)),
            pltpu.SemaphoreType.DMA((2,)),
            pltpu.SemaphoreType.DMA,
            pltpu.SemaphoreType.DMA((copies,)),
            pltpu.SemaphoreType.DMA((copies,)),
        ],
        compiler_params=pltpu.CompilerParams(
            collective_id=0, has_side_effects=True, vmem_limit_bytes=57 * 2**20,
        ),
    )(cond_table, east_class, south_class, leakage, pad_mask, load_current)


def solution(mesh):
    in_specs = (
        P("gx", "gy"),
        P("gx", "gy"),
        P(),
        P("gx", "gy"),
        P("gx", "gy"),
        P("gx", "gy", None),
    )
    out_specs = P("gx", "gy", None)
    call = functools.partial(body, mesh.shape["gx"], mesh.shape["gy"])
    return jax.shard_map(call, mesh=mesh, in_specs=in_specs, out_specs=out_specs, check_vma=False)
```

```python
import functools

import jax
import jax.numpy as jnp
from jax import lax
from jax.experimental import pallas as pl
from jax.experimental.pallas import tpu as pltpu
from jax.sharding import PartitionSpec as P

ITERS = 4
PAD_GAIN = 8.0
SPECTRAL_BOUND = 0.995
G = ITERS
MESH = pl.DeviceIdType.MESH


def polynomial():
    weights = [1.0]
    for k in range(1, ITERS):
        if k == 1:
            weights.append(1.0 / (1.0 - SPECTRAL_BOUND**2 / 2.0))
        else:
            weights.append(1.0 / (1.0 - SPECTRAL_BOUND**2 * weights[-1] / 4.0))
    size = ITERS + 1
    previous = [1.0] + [0.0] * (size - 1)
    field = [1.0, 1.0] + [0.0] * (size - 2)
    for k in range(1, ITERS):
        jac = [1.0] + field[:-1]
        updated = [weights[k] * (a - b) + b for a, b in zip(jac, previous)]
        previous, field = field, updated
    return field


def loop(lo, count, width, compute):
    def turn(start, size):
        pending = [compute(start + u) for u in range(size)]
        for stores in pending:
            for put in stores:
                put()

    turns, rest = count // width, count % width
    if turns:
        lax.fori_loop(0, turns, lambda t, c: (turn(lo + t * width, width), c)[1], 0)
    if rest:
        turn(lo + turns * width, rest)


def setter(ref, index, value):
    def put():
        ref[index] = value
    return put


EAST, SOUTH, ROOT, FLAG = range(4)


def kernel(
    nx, ny, rows, cols,
    table_hbm, east_hbm, south_hbm, leak_hbm, pad_hbm, x_ref, o_ref,
    table_ref, east_ref, south_ref, leak_ref, pad_ref,
    cf, tw, pk, pe, load, src, v1, v2, v3, bc, eload,
    small_sem, rim_sem, local_sem, send_sem, recv_sem,
):
    mx, my = lax.axis_index("gx"), lax.axis_index("gy")
    north, south = lax.rem(mx + nx - 1, nx), lax.rem(mx + 1, nx)
    west, east = lax.rem(my + ny - 1, ny), lax.rem(my + 1, ny)
    cases = x_ref.shape[2]
    halves = [slice(h * 128, (h + 1) * 128) for h in range(cases // 128)]
    poly = polynomial()

    barrier = pltpu.get_barrier_semaphore()
    peers = [(north, my), (south, my), (mx, west), (mx, east)]
    for peer in peers:
        pl.semaphore_signal(barrier, inc=1, device_id=peer, device_id_type=MESH)
    small = [
        pltpu.make_async_copy(there, here, small_sem.at[n])
        for n, (there, here) in enumerate([
            (table_hbm, table_ref), (east_hbm, east_ref), (south_hbm, south_ref),
            (leak_hbm, leak_ref), (pad_hbm, pad_ref),
        ])
    ]
    for copy in small:
        copy.start()
    area = pl.ds(G, rows)
    rims = [
        pltpu.make_async_copy(x_ref.at[:, pl.ds(0, G)], eload.at[0, area, pl.ds(G, G)], rim_sem.at[0]),
        pltpu.make_async_copy(x_ref.at[:, pl.ds(cols - G, G)], eload.at[1, area, pl.ds(0, G)], rim_sem.at[1]),
    ]
    for copy in rims:
        copy.start()
    own = pltpu.make_async_copy(x_ref, load.at[area], local_sem)
    own.start()
    for copy in small:
        copy.wait()

    def lookup(classes):
        value = jnp.full(classes.shape, table_ref[0], jnp.float32)
        for c in range(1, table_ref.shape[0]):
            value = jnp.where(classes == c, table_ref[c], value)
        return value

    blank = jnp.zeros((rows, 128 - cols), jnp.float32)
    fields = [
        lookup(east_ref[...]),
        lookup(south_ref[...]),
        leak_ref[...] + PAD_GAIN * pad_ref[...].astype(jnp.float32),
    ]
    for f in range(3):
        cf[f, pl.ds(8, rows), :] = jnp.concatenate([fields[f], blank], axis=1)

    pl.semaphore_wait(barrier, len(peers))
    for copy in rims:
        copy.wait()

    counter = [0]

    def send(source, target, device):
        n = counter[0]
        counter[0] += 1
        copy = pltpu.make_async_remote_copy(
            src_ref=source, dst_ref=target,
            send_sem=send_sem.at[n], recv_sem=recv_sem.at[n],
            device_id=device, device_id_type=MESH,
        )
        copy.start()
        return copy

    def eastward(at, count):
        rim = pl.ds(at, count), pl.ds(0, G)
        return send(eload.at[(1, *rim)], eload.at[(0, *rim)], (mx, east))

    def westward(at, count):
        rim = pl.ds(at, count), pl.ds(G, G)
        return send(eload.at[(0, *rim)], eload.at[(1, *rim)], (mx, west))

    cuts = [G + rows // 2, G + 3 * rows // 4, G + rows - 2 * G]
    mid = G + rows // 4
    ends = [eastward(G, G), westward(G, G), eastward(rows, G), westward(rows, G)]
    first = [eastward(2 * G, cuts[0] - 2 * G), westward(2 * G, mid - 2 * G)]
    cf_n = send(cf.at[:, pl.ds(rows, 8)], cf.at[:, pl.ds(0, 8)], (south, my))
    cf_s = send(cf.at[:, pl.ds(8, 8)], cf.at[:, pl.ds(rows + 8, 8)], (north, my))
    ld_n = send(x_ref.at[pl.ds(rows - G, G)], load.at[pl.ds(0, G)], (south, my))
    ld_s = send(x_ref.at[pl.ds(0, G)], load.at[pl.ds(rows + G, G)], (north, my))

    lane = lax.broadcasted_iota(jnp.int32, (8, 128), 1)

    def dense(lo, size):
        area = pl.ds(lo, size)
        e, s, extra = (cf[f, area, :] for f in range(3))
        root = lax.rsqrt(e + pltpu.roll(e, 1, 1) + s + pltpu.roll(s, 1, 0) + extra)
        flagged = jnp.where(extra > PAD_GAIN / 2, -root, root)
        left = jnp.broadcast_to(lane[0:1] < cols, (size, 128))
        after = pltpu.roll(root, size - 1, 0)
        values = [e * root * pltpu.roll(root, 127, 1), s * root * after, flagged, pltpu.roll(flagged, size - 1, 0)]
        for p in range(2):
            pk[p, area, :] = jnp.where(left, values[2 * p], pltpu.roll(values[2 * p + 1], cols, 1))

    def dense_edge(lo):
        size = 16 if lo else 24
        area = pl.ds(lo, size)
        e, s, extra = (tw[f, area, :] for f in range(3))
        e_west = tw[0, pl.ds(lo - 1, size), :] if lo else pltpu.roll(e, 1, 0)
        root = lax.rsqrt(e + e_west + s + pltpu.roll(s, 1, 1) + extra)
        flagged = jnp.where(extra > PAD_GAIN / 2, -root, root)
        values = [e * root * pltpu.roll(root, size - 1, 0), s * root * pltpu.roll(root, 127, 1), root, flagged]
        return [value[0:16] for value in values]

    def turned(ref, r):
        return jnp.transpose(jnp.broadcast_to(ref[pl.ds(r + 8 - G, 1), :], (128, 128)))

    def scaled(flagged, value):
        return jnp.abs(flagged) * (jnp.where(flagged < 0.0, PAD_GAIN, 0.0) - value)

    def spread_rows(lo, count):
        inside = pl.ds(8, cols)
        stores = []
        for r in (lo + u for u in range(0, count, 2)):
            for v in range(2):
                value = turned(pk.at[0], r + v)
                stores.append(setter(bc, (EAST, r + v, inside), value[0:cols]))
                stores.append(setter(bc, (SOUTH, r + v, inside), value[cols : 2 * cols]))
            both = turned(pk.at[1], r)
            for v in range(2):
                value = both[v * cols : (v + 1) * cols]
                stores.append(setter(bc, (ROOT, r + v, inside), jnp.abs(value)))
                for n, h in enumerate(halves):
                    stores.append(setter(src, (r + v, n, inside), scaled(value, load[r + v, :, h])))
        return stores

    def spread_edge(lo, count, width):
        def block(t):
            for u in range(width):
                r = lo + t * width + u
                value = turned(pe, r)
                for f in range(4):
                    bc[f, r, pl.ds(0, 16)] = value[32 * f : 32 * f + 16]
                    bc[f, r, pl.ds(cols, 16)] = value[32 * f + 16 : 32 * f + 32]
        lax.fori_loop(0, count // width, lambda t, c: (block(t), c)[1], 0)

    dense(8, rows)
    own.wait()
    chain = [src, v1, v2, v3]

    def gather(r, at, size):
        coefs = [
            bc[EAST, r, pl.ds(at, size)], bc[EAST, r, pl.ds(at - 1, size)],
            bc[SOUTH, r, pl.ds(at, size)], bc[SOUTH, r - 1, pl.ds(at, size)],
        ]
        return coefs

    def update(k, r, n, at, size, coefs):
        vin = chain[k - 1]
        total = coefs[0] * vin[r, n, pl.ds(at + 1, size)]
        total += coefs[1] * vin[r, n, pl.ds(at - 1, size)]
        total += coefs[2] * vin[r + 1, n, pl.ds(at, size)]
        total += coefs[3] * vin[r - 1, n, pl.ds(at, size)]
        if k == 1:
            total = total * poly[ITERS]
        total = total + poly[ITERS - k] * src[r, n, pl.ds(at, size)]
        if k == ITERS:
            total = total * bc[ROOT, r, pl.ds(at, size)]
        return total

    def step_row(k, r):
        skip = 2 * G if k == ITERS else G
        at, size = 8 + skip, cols - 2 * skip
        stores = []
        coefs = gather(r, at, size)
        for n, h in enumerate(halves):
            total = update(k, r, n, at, size, coefs)
            if k == ITERS:
                stores.append(setter(o_ref, (r - G, pl.ds(skip, size), h), total))
            else:
                stores.append(setter(chain[k], (r, n, pl.ds(at, size)), total))
        return stores

    def step(k, lo, count):
        loop(lo, count, 2, functools.partial(step_row, k))

    W = 8
    for put in spread_rows(G, W):
        put()

    def both(t):
        r = G + W + t * W
        stores = []
        for u in range(W):
            stores += step_row(1, r - W - 1 + u)
        stores += spread_rows(r, W)
        for put in stores:
            put()

    turns = rows // W - 1
    lax.fori_loop(0, turns, lambda t, c: (both(t), c)[1], 0)
    step(1, rows + G - W - 1, W)
    cf_n.wait_recv()
    cf_s.wait_recv()
    for f in range(3):
        tw[f, pl.ds(8, cols), :] = jnp.transpose(cf[f])[0:cols, :]
    tw_w = send(tw.at[:, pl.ds(cols + 2, 6)], tw.at[:, pl.ds(2, 6)], (mx, east))
    tw_e = send(tw.at[:, pl.ds(8, G)], tw.at[:, pl.ds(cols + 8, G)], (mx, west))
    second = [eastward(cuts[0], cuts[1] - cuts[0])]
    third = [eastward(cuts[1], cuts[2] - cuts[1])]
    fourth = [eastward(cuts[2], rows - cuts[2])]
    first.append(westward(mid, cuts[0] - mid))
    second.append(westward(cuts[0], cuts[1] - cuts[0]))
    third.append(westward(cuts[1], cuts[2] - cuts[1]))
    fourth.append(westward(cuts[2], rows - cuts[2]))

    for k in range(2, ITERS + 1):
        step(k, G + k + 1, rows - 2 * k - 1)

    for copy in ends:
        copy.wait_recv()
    for w in range(2):
        first.append(send(eload.at[w, pl.ds(rows, G)], eload.at[w, pl.ds(0, G)], (south, my)))
        fourth.append(send(eload.at[w, pl.ds(G, G)], eload.at[w, pl.ds(rows + G, G)], (north, my)))
    ld_n.wait_recv()
    ld_s.wait_recv()
    dense(0, rows + 16)
    for put in spread_rows(0, G + 2) + spread_rows(rows + G - 2, G + 2):
        put()
    for k in range(1, ITERS + 1):
        step(k, k, G + 1)
        step(k, rows + 2 * G - k - G, G)

    tw_w.wait_recv()
    tw_e.wait_recv()
    sides = zip(dense_edge(0), dense_edge(cols))
    pe[...] = jnp.transpose(jnp.concatenate([part for pair in sides for part in pair], axis=0))
    spread_edge(0, rows + 2 * G, 24)

    edge = 2 * G
    rims_at = [[8 - G, 9 - G, 9 - G, 10 - G, 8], [8 + cols - G, 7 + cols - G, 7 + cols - G, 6 + cols - G, 8 + cols - 2 * G]]

    def edge_source(lo, count):
        def one(r):
            stores = []
            for w in range(2):
                area = pl.ds(rims_at[w][0], edge)
                flagged = bc[FLAG, r, area]
                for n, h in enumerate(halves):
                    stores.append(setter(src, (r, n, area), scaled(flagged, eload[w, r, :, h])))
            return stores
        loop(lo, count, 4, one)

    def edge_step(k, lo, count):
        def one(r):
            stores = []
            for w in range(2):
                at = rims_at[w][k]
                coefs = gather(r, at, edge)
                for n, h in enumerate(halves):
                    total = update(k, r, n, at, edge, coefs)
                    if k < ITERS:
                        stores.append(setter(chain[k], (r, n, pl.ds(at, edge)), total))
                    else:
                        stores.append(setter(o_ref, (r - G, pl.ds(at - 8, edge), h), total))
            return stores

        loop(lo, count, 4, one)

    bounds = [0] + cuts + [rows + 2 * G]
    for m, arrived in enumerate([first, second, third, fourth]):
        for copy in arrived:
            copy.wait_recv()
        lo, hi = bounds[m], bounds[m + 1]
        edge_source(lo, hi - lo)
        for k in range(1, ITERS + 1):
            begin = k if m == 0 else lo - k
            edge_step(k, begin, hi - k - begin)
    for copy in [cf_n, cf_s, ld_n, ld_s, tw_w, tw_e] + ends + first + second + third + fourth:
        copy.wait_send()


def body(nx, ny, east_class, south_class, cond_table, leakage, pad_mask, load_current):
    rows, cols, cases = load_current.shape
    tall = rows + 2 * G
    f32 = jnp.float32
    halves = cases // 128
    anywhere = pl.BlockSpec(memory_space=pl.ANY)
    copies = 6 + 13 + 4
    grid = (tall, halves, cols + 16, 128)
    return pl.pallas_call(
        functools.partial(kernel, nx, ny, rows, cols),
        out_shape=pltpu.VMEM(load_current.shape, f32),
        in_specs=[anywhere] * 6,
        out_specs=pl.BlockSpec(memory_space=pltpu.VMEM),
        scratch_shapes=[
            pltpu.SMEM(cond_table.shape, f32),
            pltpu.VMEM((rows, cols), jnp.int32),
            pltpu.VMEM((rows, cols), jnp.int32),
            pltpu.VMEM((rows, cols), f32),
            pltpu.VMEM((rows, cols), jnp.int32),
            pltpu.VMEM((3, 128, 128), f32),
            pltpu.VMEM((3, cols + 16, 128), f32),
            pltpu.VMEM((2, 128, 128), f32),
            pltpu.VMEM((128, 128), f32),
            pltpu.VMEM((tall, cols, cases), f32),
            pltpu.VMEM(grid, f32),
            pltpu.VMEM(grid, f32),
            pltpu.VMEM(grid, f32),
            pltpu.VMEM(grid, f32),
            pltpu.VMEM((4, tall, cols + 16, 128), f32),
            pltpu.VMEM((2, tall, 2 * G, cases), f32),
            pltpu.SemaphoreType.DMA((5,)),
            pltpu.SemaphoreType.DMA((2,)),
            pltpu.SemaphoreType.DMA,
            pltpu.SemaphoreType.DMA((copies,)),
            pltpu.SemaphoreType.DMA((copies,)),
        ],
        compiler_params=pltpu.CompilerParams(
            collective_id=0, has_side_effects=True, vmem_limit_bytes=57 * 2**20,
        ),
    )(cond_table, east_class, south_class, leakage, pad_mask, load_current)


def solution(mesh):
    in_specs = (
        P("gx", "gy"),
        P("gx", "gy"),
        P(),
        P("gx", "gy"),
        P("gx", "gy"),
        P("gx", "gy", None),
    )
    out_specs = P("gx", "gy", None)
    call = functools.partial(body, mesh.shape["gx"], mesh.shape["gy"])
    return jax.shard_map(call, mesh=mesh, in_specs=in_specs, out_specs=out_specs, check_vma=False)
```

```python
import functools

import jax
import jax.numpy as jnp
from jax import lax
from jax.experimental import pallas as pl
from jax.experimental.pallas import tpu as pltpu
from jax.sharding import PartitionSpec as P

ITERS = 4
PAD_GAIN = 8.0
SPECTRAL_BOUND = 0.995
G = ITERS
MESH = pl.DeviceIdType.MESH


def polynomial():
    weights = [1.0]
    for k in range(1, ITERS):
        if k == 1:
            weights.append(1.0 / (1.0 - SPECTRAL_BOUND**2 / 2.0))
        else:
            weights.append(1.0 / (1.0 - SPECTRAL_BOUND**2 * weights[-1] / 4.0))
    size = ITERS + 1
    previous = [1.0] + [0.0] * (size - 1)
    field = [1.0, 1.0] + [0.0] * (size - 2)
    for k in range(1, ITERS):
        jac = [1.0] + field[:-1]
        updated = [weights[k] * (a - b) + b for a, b in zip(jac, previous)]
        previous, field = field, updated
    return field


def loop(lo, count, width, compute):
    def turn(start, size):
        pending = [compute(start + u) for u in range(size)]
        for stores in pending:
            for put in stores:
                put()

    turns, rest = count // width, count % width
    if turns:
        lax.fori_loop(0, turns, lambda t, c: (turn(lo + t * width, width), c)[1], 0)
    if rest:
        turn(lo + turns * width, rest)


def setter(ref, index, value):
    def put():
        ref[index] = value
    return put


EAST, SOUTH, ROOT, FLAG = range(4)


def kernel(
    nx, ny, rows, cols,
    table_hbm, east_hbm, south_hbm, leak_hbm, pad_hbm, x_ref, o_ref,
    table_ref, east_ref, south_ref, leak_ref, pad_ref,
    cf, tw, passing, pk, pe, load, src, v1, v2, v3, bc, eload,
    small_sem, rim_sem, local_sem, send_sem, recv_sem,
):
    mx, my = lax.axis_index("gx"), lax.axis_index("gy")
    north, south = lax.rem(mx + nx - 1, nx), lax.rem(mx + 1, nx)
    west, east = lax.rem(my + ny - 1, ny), lax.rem(my + 1, ny)
    cases = x_ref.shape[2]
    halves = [slice(h * 128, (h + 1) * 128) for h in range(cases // 128)]
    poly = polynomial()

    barrier = pltpu.get_barrier_semaphore()
    peers = [(north, my), (south, my), (mx, west), (mx, east)]
    for peer in peers:
        pl.semaphore_signal(barrier, inc=1, device_id=peer, device_id_type=MESH)
    small = [
        pltpu.make_async_copy(there, here, small_sem.at[n])
        for n, (there, here) in enumerate([
            (table_hbm, table_ref), (east_hbm, east_ref), (south_hbm, south_ref),
            (leak_hbm, leak_ref), (pad_hbm, pad_ref),
        ])
    ]
    for copy in small:
        copy.start()
    area = pl.ds(G, rows)
    rims = [
        pltpu.make_async_copy(x_ref.at[:, pl.ds(0, G)], eload.at[0, area, pl.ds(G, G)], rim_sem.at[0]),
        pltpu.make_async_copy(x_ref.at[:, pl.ds(cols - G, G)], eload.at[1, area, pl.ds(0, G)], rim_sem.at[1]),
    ]
    for copy in rims:
        copy.start()
    borders = [
        pltpu.make_async_copy(x_ref.at[pl.ds(at, G)], load.at[pl.ds(at + G, G)], rim_sem.at[2 + n])
        for n, at in enumerate([0, rows - G])
    ]
    rims += borders
    for copy in borders:
        copy.start()
    own = pltpu.make_async_copy(x_ref.at[pl.ds(G, rows - 2 * G)], load.at[pl.ds(2 * G, rows - 2 * G)], local_sem)
    own.start()
    for copy in small:
        copy.wait()

    def lookup(classes):
        value = jnp.full(classes.shape, table_ref[0], jnp.float32)
        for c in range(1, table_ref.shape[0]):
            value = jnp.where(classes == c, table_ref[c], value)
        return value

    blank = jnp.zeros((rows, 128 - cols), jnp.float32)
    fields = [
        lookup(east_ref[...]),
        lookup(south_ref[...]),
        leak_ref[...] + PAD_GAIN * pad_ref[...].astype(jnp.float32),
    ]
    for f in range(3):
        cf[f, pl.ds(8, rows), :] = jnp.concatenate([fields[f], blank], axis=1)

    lane = lax.broadcasted_iota(jnp.int32, (8, 128), 1)

    def transposed(f):
        return jnp.transpose(cf[f])[0:cols, :]

    def dense(lo, size):
        area = pl.ds(lo, size)
        e, s, extra = (cf[f, area, :] for f in range(3))
        root = lax.rsqrt(e + pltpu.roll(e, 1, 1) + s + pltpu.roll(s, 1, 0) + extra)
        flagged = jnp.where(extra > PAD_GAIN / 2, -root, root)
        left = jnp.broadcast_to(lane[0:1] < cols, (size, 128))
        after = pltpu.roll(root, size - 1, 0)
        values = [e * root * pltpu.roll(root, 127, 1), s * root * after, flagged, pltpu.roll(flagged, size - 1, 0)]
        for p in range(2):
            pk[p, area, :] = jnp.where(left, values[2 * p], pltpu.roll(values[2 * p + 1], cols, 1))

    def dense_edge(w, corners):
        values = []
        wide = jnp.broadcast_to(lane[0:1], (8, 128))
        for f in range(3):
            whole = transposed(f)
            ghost = tw[f, pl.ds(w * (cols + 8), 8), :]
            if corners:
                ghost = jnp.where(wide < 8, pltpu.roll(passing[0, f, pl.ds(8 * w, 8), :], 128 - rows, 1), ghost)
                ghost = jnp.where(wide < rows + 8, ghost, pltpu.roll(passing[1, f, pl.ds(8 * w, 8), :], rows, 1))
            parts = [whole[cols - 16 :], ghost] if w else [ghost, whole[0:16]]
            values.append(jnp.concatenate(parts, axis=0))
        e, s, extra = values
        root = lax.rsqrt(e + pltpu.roll(e, 1, 0) + s + pltpu.roll(s, 1, 1) + extra)
        flagged = jnp.where(extra > PAD_GAIN / 2, -root, root)
        values = [e * root * pltpu.roll(root, 23, 0), s * root * pltpu.roll(root, 127, 1), root, flagged]
        return [value[8 * w : 8 * w + 16] for value in values]

    def turned(ref, r):
        return jnp.transpose(jnp.broadcast_to(ref[pl.ds(r + 8 - G, 1), :], (128, 128)))

    def scaled(flagged, value):
        return jnp.abs(flagged) * (jnp.where(flagged < 0.0, PAD_GAIN, 0.0) - value)

    def spread_rows(lo, count, loaded=True):
        inside = pl.ds(8, cols)
        stores = []
        for r in (lo + u for u in range(0, count, 2)):
            for v in range(2):
                value = turned(pk.at[0], r + v)
                stores.append(setter(bc, (EAST, r + v, inside), value[0:cols]))
                stores.append(setter(bc, (SOUTH, r + v, inside), value[cols : 2 * cols]))
            both = turned(pk.at[1], r)
            for v in range(2):
                value = both[v * cols : (v + 1) * cols]
                stores.append(setter(bc, (ROOT, r + v, inside), jnp.abs(value)))
                if not loaded:
                    stores.append(setter(bc, (FLAG, r + v, inside), value))
                    continue
                for n, h in enumerate(halves):
                    stores.append(setter(src, (r + v, n, inside), scaled(value, load[r + v, :, h])))
        return stores

    def spread_edge(lo, count, width):
        def block(t):
            for u in range(width):
                r = lo + t * width + u
                value = turned(pe, r)
                for f in range(4):
                    bc[f, r, pl.ds(0, 16)] = value[32 * f : 32 * f + 16]
                    bc[f, r, pl.ds(cols, 16)] = value[32 * f + 16 : 32 * f + 32]
        lax.fori_loop(0, count // width, lambda t, c: (block(t), c)[1], 0)

    above, below = jnp.zeros((8, 128), jnp.float32), jnp.zeros((120 - rows, 128), jnp.float32)
    for f in range(3):
        square = jnp.concatenate([above, jnp.concatenate([fields[f], blank], axis=1), below], axis=0)
        tw[f, pl.ds(8, cols), :] = jnp.transpose(square)[0:cols, :]
    dense(8, rows)
    early = 16
    for put in spread_rows(G, early, False):
        put()

    pl.semaphore_wait(barrier, len(peers))
    for copy in rims:
        copy.wait()

    counter = [0]

    def send(source, target, device):
        n = counter[0]
        counter[0] += 1
        copy = pltpu.make_async_remote_copy(
            src_ref=source, dst_ref=target,
            send_sem=send_sem.at[n], recv_sem=recv_sem.at[n],
            device_id=device, device_id_type=MESH,
        )
        copy.start()
        return copy

    def eastward(at, count):
        rim = pl.ds(at, count), pl.ds(0, G)
        return send(eload.at[(1, *rim)], eload.at[(0, *rim)], (mx, east))

    def westward(at, count):
        rim = pl.ds(at, count), pl.ds(G, G)
        return send(eload.at[(0, *rim)], eload.at[(1, *rim)], (mx, west))

    cuts = [G + rows // 4, G + rows // 2, G + 3 * rows // 4, G + rows - 2 * G, rows + 2 * G]
    heads = [2 * G] + cuts[:-1]
    spans = [(lo, min(hi, rows) - lo) for lo, hi in zip(heads, cuts)]
    tw_w = send(tw.at[:, pl.ds(cols + 2, 6)], tw.at[:, pl.ds(2, 6)], (mx, east))
    tw_e = send(tw.at[:, pl.ds(8, G)], tw.at[:, pl.ds(cols + 8, G)], (mx, west))
    ends = [way(at, G) for way in (eastward, westward) for at in (G, rows)]
    arrivals = [[eastward(*span)] for span in spans]
    for part, span in zip(arrivals, spans):
        part.append(westward(*span))
    cf_n = send(cf.at[:, pl.ds(rows, 8)], cf.at[:, pl.ds(0, 8)], (south, my))
    cf_s = send(cf.at[:, pl.ds(8, 8)], cf.at[:, pl.ds(rows + 8, 8)], (north, my))
    ld_n = send(load.at[pl.ds(rows, G)], load.at[pl.ds(0, G)], (south, my))
    ld_s = send(load.at[pl.ds(G, G)], load.at[pl.ds(rows + G, G)], (north, my))

    chain = [src, v1, v2, v3]

    def gather(r, at, size):
        coefs = [
            bc[EAST, r, pl.ds(at, size)], bc[EAST, r, pl.ds(at - 1, size)],
            bc[SOUTH, r, pl.ds(at, size)], bc[SOUTH, r - 1, pl.ds(at, size)],
        ]
        return coefs

    def update(k, r, n, at, size, coefs):
        vin = chain[k - 1]
        total = coefs[0] * vin[r, n, pl.ds(at + 1, size)]
        total += coefs[1] * vin[r, n, pl.ds(at - 1, size)]
        total += coefs[2] * vin[r + 1, n, pl.ds(at, size)]
        total += coefs[3] * vin[r - 1, n, pl.ds(at, size)]
        if k == 1:
            total = total * poly[ITERS]
        total = total + poly[ITERS - k] * src[r, n, pl.ds(at, size)]
        if k == ITERS:
            total = total * bc[ROOT, r, pl.ds(at, size)]
        return total

    def step_row(k, r):
        skip = 2 * G if k == ITERS else G
        at, size = 8 + skip, cols - 2 * skip
        stores = []
        coefs = gather(r, at, size)
        for n, h in enumerate(halves):
            total = update(k, r, n, at, size, coefs)
            if k == ITERS:
                stores.append(setter(o_ref, (r - G, pl.ds(skip, size), h), total))
            else:
                stores.append(setter(chain[k], (r, n, pl.ds(at, size)), total))
        return stores

    def step(k, lo, count):
        loop(lo, count, 2, functools.partial(step_row, k))

    own.wait()

    def source_row(r):
        inside = pl.ds(8, cols)
        flagged = bc[FLAG, r, inside]
        return [setter(src, (r, n, inside), scaled(flagged, load[r, :, h])) for n, h in enumerate(halves)]

    loop(G, early, 2, source_row)
    W = 8

    def both(t):
        r = G + early + t * W
        stores = []
        for u in range(W):
            stores += step_row(1, r - W - 1 + u)
        stores += spread_rows(r, W)
        for put in stores:
            put()

    if early > W:
        step(1, G + 2, early - W - 3)
    turns = (rows - early) // W
    lax.fori_loop(0, turns, lambda t, c: (both(t), c)[1], 0)
    step(1, rows + G - W - 1, W)
    for k in range(2, ITERS + 1):
        step(k, G + k + 1, rows - 2 * k - 1)
        if k == 2:
            tw_w.wait_recv()
            tw_e.wait_recv()
            passed = [
                send(tw.at[:, pl.ds(at, 8)], passing.at[n, :, pl.ds(8 * w, 8)], (peer, my))
                for n, peer in enumerate([south, north])
                for w, at in enumerate([0, cols + 8])
            ]
            for copy in ends:
                copy.wait_recv()
            for w in range(2):
                arrivals[0].append(send(eload.at[w, pl.ds(rows, G)], eload.at[w, pl.ds(0, G)], (south, my)))
                arrivals[-1].append(send(eload.at[w, pl.ds(G, G)], eload.at[w, pl.ds(rows + G, G)], (north, my)))

    cf_n.wait_recv()
    cf_s.wait_recv()
    dense(0, rows + 16)
    for put in spread_rows(0, G + 2, False) + spread_rows(rows + G - 2, G + 2, False):
        put()

    def edge_fields(corners):
        sides = zip(dense_edge(0, corners), dense_edge(1, corners))
        pe[...] = jnp.transpose(jnp.concatenate([part for pair in sides for part in pair], axis=0))

    edge_fields(False)
    spread_edge(2 * G, rows - 2 * G, 28)

    ld_n.wait_recv()
    ld_s.wait_recv()
    loop(0, G + 1, 2, source_row)
    loop(rows + G, G, 2, source_row)
    for k in range(1, ITERS + 1):
        step(k, k, G + 1)
        step(k, rows + 2 * G - k - G, G)
    for copy in passed:
        copy.wait_recv()
    edge_fields(True)
    spread_edge(0, 2 * G, 2 * G)
    spread_edge(rows, 2 * G, 2 * G)

    edge = 2 * G
    rims_at = [[8 - G, 9 - G, 9 - G, 10 - G, 8], [8 + cols - G, 7 + cols - G, 7 + cols - G, 6 + cols - G, 8 + cols - 2 * G]]

    def edge_source(lo, count):
        def one(r):
            stores = []
            for w in range(2):
                area = pl.ds(rims_at[w][0], edge)
                flagged = bc[FLAG, r, area]
                for n, h in enumerate(halves):
                    stores.append(setter(src, (r, n, area), scaled(flagged, eload[w, r, :, h])))
            return stores
        loop(lo, count, 4, one)

    def edge_step(k, lo, count):
        def one(r):
            stores = []
            for w in range(2):
                at = rims_at[w][k]
                coefs = gather(r, at, edge)
                for n, h in enumerate(halves):
                    total = update(k, r, n, at, edge, coefs)
                    if k < ITERS:
                        stores.append(setter(chain[k], (r, n, pl.ds(at, edge)), total))
                    else:
                        stores.append(setter(o_ref, (r - G, pl.ds(at - 8, edge), h), total))
            return stores

        loop(lo, count, 4, one)

    bounds = [0] + cuts
    for m, arrived in enumerate(arrivals):
        for copy in arrived:
            copy.wait_recv()
        lo, hi = bounds[m], bounds[m + 1]
        edge_source(lo, hi - lo)
        for k in range(1, ITERS + 1):
            begin = k if m == 0 else lo - k
            edge_step(k, begin, hi - k - begin)
    for copy in [cf_n, cf_s, ld_n, ld_s, tw_w, tw_e] + passed + ends + sum(arrivals, []):
        copy.wait_send()


def body(nx, ny, east_class, south_class, cond_table, leakage, pad_mask, load_current):
    rows, cols, cases = load_current.shape
    tall = rows + 2 * G
    f32 = jnp.float32
    halves = cases // 128
    anywhere = pl.BlockSpec(memory_space=pl.ANY)
    copies = 6 + 4 + 10 + 8
    grid = (tall, halves, cols + 16, 128)
    return pl.pallas_call(
        functools.partial(kernel, nx, ny, rows, cols),
        out_shape=pltpu.VMEM(load_current.shape, f32),
        in_specs=[anywhere] * 6,
        out_specs=pl.BlockSpec(memory_space=pltpu.VMEM),
        scratch_shapes=[
            pltpu.SMEM(cond_table.shape, f32),
            pltpu.VMEM((rows, cols), jnp.int32),
            pltpu.VMEM((rows, cols), jnp.int32),
            pltpu.VMEM((rows, cols), f32),
            pltpu.VMEM((rows, cols), jnp.int32),
            pltpu.VMEM((3, 128, 128), f32),
            pltpu.VMEM((3, cols + 16, 128), f32),
            pltpu.VMEM((2, 3, 16, 128), f32),
            pltpu.VMEM((2, 128, 128), f32),
            pltpu.VMEM((128, 128), f32),
            pltpu.VMEM((tall, cols, cases), f32),
            pltpu.VMEM(grid, f32),
            pltpu.VMEM(grid, f32),
            pltpu.VMEM(grid, f32),
            pltpu.VMEM(grid, f32),
            pltpu.VMEM((4, tall, cols + 16, 128), f32),
            pltpu.VMEM((2, tall, 2 * G, cases), f32),
            pltpu.SemaphoreType.DMA((5,)),
            pltpu.SemaphoreType.DMA((4,)),
            pltpu.SemaphoreType.DMA,
            pltpu.SemaphoreType.DMA((copies,)),
            pltpu.SemaphoreType.DMA((copies,)),
        ],
        compiler_params=pltpu.CompilerParams(
            collective_id=0, has_side_effects=True, vmem_limit_bytes=57 * 2**20,
        ),
    )(cond_table, east_class, south_class, leakage, pad_mask, load_current)


def solution(mesh):
    in_specs = (
        P("gx", "gy"),
        P("gx", "gy"),
        P(),
        P("gx", "gy"),
        P("gx", "gy"),
        P("gx", "gy", None),
    )
    out_specs = P("gx", "gy", None)
    call = functools.partial(body, mesh.shape["gx"], mesh.shape["gy"])
    return jax.shard_map(call, mesh=mesh, in_specs=in_specs, out_specs=out_specs, check_vma=False)
```

```python
import functools

import jax
import jax.numpy as jnp
from jax import lax
from jax.experimental import pallas as pl
from jax.experimental.pallas import tpu as pltpu
from jax.sharding import PartitionSpec as P

ITERS = 4
PAD_GAIN = 8.0
SPECTRAL_BOUND = 0.995
G = ITERS
MESH = pl.DeviceIdType.MESH


def polynomial():
    weights = [1.0]
    for k in range(1, ITERS):
        if k == 1:
            weights.append(1.0 / (1.0 - SPECTRAL_BOUND**2 / 2.0))
        else:
            weights.append(1.0 / (1.0 - SPECTRAL_BOUND**2 * weights[-1] / 4.0))
    size = ITERS + 1
    previous = [1.0] + [0.0] * (size - 1)
    field = [1.0, 1.0] + [0.0] * (size - 2)
    for k in range(1, ITERS):
        jac = [1.0] + field[:-1]
        updated = [weights[k] * (a - b) + b for a, b in zip(jac, previous)]
        previous, field = field, updated
    return field


def loop(lo, count, width, compute):
    def turn(start, size):
        pending = [compute(start + u) for u in range(size)]
        for stores in pending:
            for put in stores:
                put()

    turns, rest = count // width, count % width
    if turns:
        lax.fori_loop(0, turns, lambda t, c: (turn(lo + t * width, width), c)[1], 0)
    if rest:
        turn(lo + turns * width, rest)


def setter(ref, index, value):
    def put():
        ref[index] = value
    return put


EAST, SOUTH, ROOT, FLAG = range(4)


def kernel(
    nx, ny, rows, cols,
    table_hbm, east_hbm, south_hbm, leak_hbm, pad_hbm, x_ref, o_ref,
    table_ref, east_ref, south_ref, leak_ref, pad_ref,
    cf, tw, passing, rim, pk, pe, load, src, v1, v2, v3, bc, eload,
    small_sem, rim_sem, local_sem, send_sem, recv_sem,
):
    mx, my = lax.axis_index("gx"), lax.axis_index("gy")
    north, south = lax.rem(mx + nx - 1, nx), lax.rem(mx + 1, nx)
    west, east = lax.rem(my + ny - 1, ny), lax.rem(my + 1, ny)
    cases = x_ref.shape[2]
    halves = [slice(h * 128, (h + 1) * 128) for h in range(cases // 128)]
    poly = polynomial()

    def settle(view, semaphore):
        pltpu.make_async_copy(view, view, semaphore).wait()

    barrier = pltpu.get_barrier_semaphore()
    peers = [(north, my), (south, my), (mx, west), (mx, east)]
    for peer in peers:
        pl.semaphore_signal(barrier, inc=1, device_id=peer, device_id_type=MESH)
    small = [
        pltpu.make_async_copy(there, here, small_sem.at[n])
        for n, (there, here) in enumerate([
            (table_hbm, table_ref), (east_hbm, east_ref), (south_hbm, south_ref),
            (leak_hbm, leak_ref), (pad_hbm, pad_ref),
        ])
    ]
    for copy in small:
        copy.start()
    area = pl.ds(G, rows)
    rims = [
        pltpu.make_async_copy(x_ref.at[:, pl.ds(0, G)], eload.at[0, area, pl.ds(G, G)], rim_sem),
        pltpu.make_async_copy(x_ref.at[:, pl.ds(cols - G, G)], eload.at[1, area, pl.ds(0, G)], rim_sem),
    ]
    for copy in rims:
        copy.start()
    borders = [
        pltpu.make_async_copy(x_ref.at[pl.ds(at, G)], load.at[pl.ds(at + G, G)], rim_sem)
        for at in [0, rows - G]
    ]
    rims += borders
    for copy in borders:
        copy.start()
    own = pltpu.make_async_copy(x_ref.at[pl.ds(G, rows - 2 * G)], load.at[pl.ds(2 * G, rows - 2 * G)], local_sem)
    own.start()
    for copy in small:
        copy.wait()

    def lookup(classes):
        value = jnp.full(classes.shape, table_ref[0], jnp.float32)
        for c in range(1, table_ref.shape[0]):
            value = jnp.where(classes == c, table_ref[c], value)
        return value

    blank = jnp.zeros((rows, 128 - cols), jnp.float32)
    fields = [
        lookup(east_ref[...]),
        lookup(south_ref[...]),
        leak_ref[...] + PAD_GAIN * pad_ref[...].astype(jnp.float32),
    ]
    for f in range(3):
        cf[f, pl.ds(8, rows), :] = jnp.concatenate([fields[f], blank], axis=1)

    lane = lax.broadcasted_iota(jnp.int32, (8, 128), 1)

    def transposed(f):
        return jnp.transpose(cf[f])[0:cols, :]

    def dense(lo, size):
        area = pl.ds(lo, size)
        e, s, extra = (cf[f, area, :] for f in range(3))
        root = lax.rsqrt(e + pltpu.roll(e, 1, 1) + s + pltpu.roll(s, 1, 0) + extra)
        flagged = jnp.where(extra > PAD_GAIN / 2, -root, root)
        left = jnp.broadcast_to(lane[0:1] < cols, (size, 128))
        after = pltpu.roll(root, size - 1, 0)
        values = [e * root * pltpu.roll(root, 127, 1), s * root * after, flagged, pltpu.roll(flagged, size - 1, 0)]
        for p in range(2):
            pk[p, area, :] = jnp.where(left, values[2 * p], pltpu.roll(values[2 * p + 1], cols, 1))

    def dense_edge(w, corners):
        values = []
        wide = jnp.broadcast_to(lane[0:1], (8, 128))
        for f in range(3):
            ghost = tw[f, pl.ds(w * (cols + 8), 8), :]
            if corners:
                ghost = jnp.where(wide < 8, pltpu.roll(passing[0, f, pl.ds(8 * w, 8), :], 128 - rows, 1), ghost)
                ghost = jnp.where(wide < rows + 8, ghost, pltpu.roll(passing[1, f, pl.ds(8 * w, 8), :], rows, 1))
            own_side = rim[f, pl.ds(16 * w, 16), :]
            values.append(jnp.concatenate([own_side, ghost] if w else [ghost, own_side], axis=0))
        e, s, extra = values
        root = lax.rsqrt(e + pltpu.roll(e, 1, 0) + s + pltpu.roll(s, 1, 1) + extra)
        flagged = jnp.where(extra > PAD_GAIN / 2, -root, root)
        values = [e * root * pltpu.roll(root, 23, 0), s * root * pltpu.roll(root, 127, 1), flagged]
        first = 16 - G if w else 8 - G
        return [value[first : first + 2 * G] for value in values]

    def turned(ref, r):
        return jnp.transpose(jnp.broadcast_to(ref[pl.ds(r + 8 - G, 1), :], (128, 128)))

    def scaled(flagged, value):
        return jnp.abs(flagged) * (jnp.where(flagged < 0.0, PAD_GAIN, 0.0) - value)

    def spread_rows(lo, count, loaded=True):
        inside = pl.ds(8, cols)
        stores = []
        for r in (lo + u for u in range(0, count, 2)):
            for v in range(2):
                value = turned(pk.at[0], r + v)
                stores.append(setter(bc, (EAST, r + v, inside), value[0:cols]))
                stores.append(setter(bc, (SOUTH, r + v, inside), value[cols : 2 * cols]))
            both = turned(pk.at[1], r)
            for v in range(2):
                value = both[v * cols : (v + 1) * cols]
                stores.append(setter(bc, (ROOT, r + v, inside), jnp.abs(value) * poly[ITERS]))
                if not loaded:
                    stores.append(setter(bc, (FLAG, r + v, inside), value))
                    continue
                for n, h in enumerate(halves):
                    stores.append(setter(src, (r + v, n, inside), scaled(value, load[r + v, :, h])))
        return stores

    def spread_edge(lo, count, width):
        def block(t):
            for u in range(0, width, 2):
                r = lo + t * width + u
                value = turned(pe, r)
                for v in range(2):
                    for w, at in enumerate([8 - G, 8 + cols - G]):
                        area = pl.ds(at, 2 * G)
                        e, s, flagged = (value[64 * v + 8 * (3 * w + f) :][: 2 * G] for f in range(3))
                        bc[EAST, r + v, area] = e
                        bc[SOUTH, r + v, area] = s
                        bc[FLAG, r + v, area] = flagged
                        bc[ROOT, r + v, area] = jnp.abs(flagged) * poly[ITERS]
        lax.fori_loop(0, count // width, lambda t, c: (block(t), c)[1], 0)

    above, below = jnp.zeros((8, 128), jnp.float32), jnp.zeros((120 - rows, 128), jnp.float32)
    for f in range(3):
        square = jnp.concatenate([above, jnp.concatenate([fields[f], blank], axis=1), below], axis=0)
        tw[f, pl.ds(8, cols), :] = jnp.transpose(square)[0:cols, :]
    dense(8, rows)
    early = 16
    for put in spread_rows(G, early, False):
        put()

    pl.semaphore_wait(barrier, len(peers))
    settle(load.at[pl.ds(0, 4 * G)], rim_sem)

    def send(source, target, device, group, bulk=1):
        copy = pltpu.make_async_remote_copy(
            src_ref=source, dst_ref=target,
            send_sem=send_sem.at[bulk], recv_sem=recv_sem.at[group],
            device_id=device, device_id_type=MESH,
        )
        copy.start()

    def eastward(at, count, group):
        part = pl.ds(at, count), pl.ds(0, G)
        send(eload.at[(1, *part)], eload.at[(0, *part)], (mx, east), group)

    def westward(at, count, group):
        part = pl.ds(at, count), pl.ds(G, G)
        send(eload.at[(0, *part)], eload.at[(1, *part)], (mx, west), group)

    cuts = [G + rows * part // 8 for part in (2, 4, 5, 6, 7)] + [rows]
    heads = [2 * G] + cuts[:-1]
    spans = [(lo, hi - lo) for lo, hi in zip(heads, cuts)]
    send(tw.at[:, pl.ds(cols + 2, 6)], tw.at[:, pl.ds(2, 6)], (mx, east), 0, 0)
    send(tw.at[:, pl.ds(8, G)], tw.at[:, pl.ds(cols + 8, G)], (mx, west), 0, 0)
    for way in (eastward, westward):
        way(G, G, 1)
        way(rows, G, 1)
    for way in (eastward, westward):
        for n, span in enumerate(spans):
            way(*span, 5 + n)
    send(cf.at[:, pl.ds(rows, 8)], cf.at[:, pl.ds(0, 8)], (south, my), 2, 0)
    send(cf.at[:, pl.ds(8, 8)], cf.at[:, pl.ds(rows + 8, 8)], (north, my), 2, 0)
    send(load.at[pl.ds(rows, G)], load.at[pl.ds(0, G)], (south, my), 3)
    send(load.at[pl.ds(G, G)], load.at[pl.ds(rows + G, G)], (north, my), 3)

    chain = [src, v1, v2, v3]

    def gather(r, at, size):
        coefs = [
            bc[EAST, r, pl.ds(at, size)], bc[EAST, r, pl.ds(at - 1, size)],
            bc[SOUTH, r, pl.ds(at, size)], bc[SOUTH, r - 1, pl.ds(at, size)],
        ]
        return coefs

    def update(k, r, n, at, size, coefs):
        vin = chain[k - 1]
        total = coefs[0] * vin[r, n, pl.ds(at + 1, size)]
        total += coefs[1] * vin[r, n, pl.ds(at - 1, size)]
        total += coefs[2] * vin[r + 1, n, pl.ds(at, size)]
        total += coefs[3] * vin[r - 1, n, pl.ds(at, size)]
        total = total + poly[ITERS - k] / poly[ITERS] * src[r, n, pl.ds(at, size)]
        if k == ITERS:
            total = total * bc[ROOT, r, pl.ds(at, size)]
        return total

    def step_row(k, r):
        skip = 2 * G if k == ITERS else G
        at, size = 8 + skip, cols - 2 * skip
        stores = []
        coefs = gather(r, at, size)
        for n, h in enumerate(halves):
            total = update(k, r, n, at, size, coefs)
            if k == ITERS:
                stores.append(setter(o_ref, (r - G, pl.ds(skip, size), h), total))
            else:
                stores.append(setter(chain[k], (r, n, pl.ds(at, size)), total))
        return stores

    def step(k, lo, count):
        loop(lo, count, 2, functools.partial(step_row, k))

    own.wait()

    def source_row(r):
        inside = pl.ds(8, cols)
        flagged = bc[FLAG, r, inside]
        return [setter(src, (r, n, inside), scaled(flagged, load[r, :, h])) for n, h in enumerate(halves)]

    loop(G, early, 2, source_row)
    W = 8

    def both(t):
        r = G + early + t * W
        stores = []
        for u in range(W):
            stores += step_row(1, r - W - 1 + u)
        stores += spread_rows(r, W)
        for put in stores:
            put()

    if early > W:
        step(1, G + 2, early - W - 3)
    turns = (rows - early) // W
    lax.fori_loop(0, turns, lambda t, c: (both(t), c)[1], 0)
    step(1, rows + G - W - 1, W)
    for k in range(2, ITERS + 1):
        step(k, G + k + 1, rows - 2 * k - 1)
        if k == 2:
            settle(cf.at[:, pl.ds(0, 6 + G)], recv_sem.at[0])
            for n, peer in enumerate([south, north]):
                for w, at in enumerate([0, cols + 8]):
                    send(tw.at[:, pl.ds(at, 8)], passing.at[n, :, pl.ds(8 * w, 8)], (peer, my), 4, 0)
            settle(eload.at[0, pl.ds(0, 2 * G)], recv_sem.at[1])
            for w in range(2):
                send(eload.at[w, pl.ds(rows, G)], eload.at[w, pl.ds(0, G)], (south, my), 5)
                send(eload.at[w, pl.ds(G, G)], eload.at[w, pl.ds(rows + G, G)], (north, my), 5)

    settle(cf.at[:, pl.ds(0, 16)], recv_sem.at[2])
    dense(0, rows + 16)
    for put in spread_rows(0, G + 2, False) + spread_rows(rows + G - 2, G + 2, False):
        put()

    def edge_fields(corners):
        stack = jnp.concatenate(dense_edge(0, corners) + dense_edge(1, corners) + [jnp.zeros((16, 128), jnp.float32)], axis=0)
        pe[...] = jnp.transpose(jnp.concatenate([stack, pltpu.roll(stack, 127, 1)], axis=0))

    for f in range(3):
        whole = transposed(f)
        rim[f] = jnp.concatenate([whole[0:16], whole[cols - 16 :]], axis=0)
    edge_fields(False)
    spread_edge(2 * G, rows - 2 * G, 28)

    settle(load.at[pl.ds(0, 2 * G)], recv_sem.at[3])
    loop(0, G + 1, 2, source_row)
    loop(rows + G, G, 2, source_row)
    for k in range(1, ITERS + 1):
        step(k, k, G + 1)
        step(k, rows + 2 * G - k - G, G)
    settle(cf.at[:, pl.ds(0, 32)], recv_sem.at[4])
    edge_fields(True)
    spread_edge(0, 2 * G, 2 * G)
    spread_edge(rows, 2 * G, 2 * G)

    edge = 2 * G
    rims_at = [[8 - G, 9 - G, 9 - G, 10 - G, 8], [8 + cols - G, 7 + cols - G, 7 + cols - G, 6 + cols - G, 8 + cols - 2 * G]]

    def edge_source(lo, count):
        def one(r):
            stores = []
            for w in range(2):
                area = pl.ds(rims_at[w][0], edge)
                flagged = bc[FLAG, r, area]
                for n, h in enumerate(halves):
                    stores.append(setter(src, (r, n, area), scaled(flagged, eload[w, r, :, h])))
            return stores
        loop(lo, count, 4, one)

    def edge_step(k, lo, count):
        def one(r):
            stores = []
            for w in range(2):
                at = rims_at[w][k]
                coefs = gather(r, at, edge)
                for n, h in enumerate(halves):
                    total = update(k, r, n, at, edge, coefs)
                    if k < ITERS:
                        stores.append(setter(chain[k], (r, n, pl.ds(at, edge)), total))
                    else:
                        stores.append(setter(o_ref, (r - G, pl.ds(at - 8, edge), h), total))
            return stores

        loop(lo, count, 4, one)

    bounds = [0] + cuts
    for m, (_, count) in enumerate(spans):
        settle(eload.at[0, pl.ds(0, count if m else count + 4 * G)], recv_sem.at[5 + m])
        lo, hi = bounds[m], bounds[m + 1]
        last = m == len(spans) - 1
        edge_source(lo, hi - lo)
        for k in range(1, ITERS + 1):
            begin = k if m == 0 else lo - k
            edge_step(k, begin, (hi + k if last else hi - k) - begin)
        if m == 0:
            edge_source(rows, 2 * G)
            for k in range(1, G):
                edge_step(k, rows + k, 2 * G - 2 * k)
    settle(cf.at[:, pl.ds(0, 6 + G + 16 + 32)], send_sem.at[0])
    sent = 2 * rows * G + 2 * G * cols + 4 * G * 2 * G
    settle(load.at[pl.ds(0, sent // cols)], send_sem.at[1])


def body(nx, ny, east_class, south_class, cond_table, leakage, pad_mask, load_current):
    rows, cols, cases = load_current.shape
    tall = rows + 2 * G
    f32 = jnp.float32
    halves = cases // 128
    anywhere = pl.BlockSpec(memory_space=pl.ANY)
    grid = (tall, halves, cols + 16, 128)
    return pl.pallas_call(
        functools.partial(kernel, nx, ny, rows, cols),
        out_shape=pltpu.VMEM(load_current.shape, f32),
        in_specs=[anywhere] * 6,
        out_specs=pl.BlockSpec(memory_space=pltpu.VMEM),
        scratch_shapes=[
            pltpu.SMEM(cond_table.shape, f32),
            pltpu.VMEM((rows, cols), jnp.int32),
            pltpu.VMEM((rows, cols), jnp.int32),
            pltpu.VMEM((rows, cols), f32),
            pltpu.VMEM((rows, cols), jnp.int32),
            pltpu.VMEM((3, 128, 128), f32),
            pltpu.VMEM((3, cols + 16, 128), f32),
            pltpu.VMEM((2, 3, 16, 128), f32),
            pltpu.VMEM((3, 32, 128), f32),
            pltpu.VMEM((2, 128, 128), f32),
            pltpu.VMEM((128, 128), f32),
            pltpu.VMEM((tall, cols, cases), f32),
            pltpu.VMEM(grid, f32),
            pltpu.VMEM(grid, f32),
            pltpu.VMEM(grid, f32),
            pltpu.VMEM(grid, f32),
            pltpu.VMEM((4, tall, cols + 16, 128), f32),
            pltpu.VMEM((2, tall, 2 * G, cases), f32),
            pltpu.SemaphoreType.DMA((5,)),
            pltpu.SemaphoreType.DMA,
            pltpu.SemaphoreType.DMA,
            pltpu.SemaphoreType.DMA((2,)),
            pltpu.SemaphoreType.DMA((11,)),
        ],
        compiler_params=pltpu.CompilerParams(
            collective_id=0, has_side_effects=True, vmem_limit_bytes=57 * 2**20,
        ),
    )(cond_table, east_class, south_class, leakage, pad_mask, load_current)


def solution(mesh):
    in_specs = (
        P("gx", "gy"),
        P("gx", "gy"),
        P(),
        P("gx", "gy"),
        P("gx", "gy"),
        P("gx", "gy", None),
    )
    out_specs = P("gx", "gy", None)
    call = functools.partial(body, mesh.shape["gx"], mesh.shape["gy"])
    return jax.shard_map(call, mesh=mesh, in_specs=in_specs, out_specs=out_specs, check_vma=False)
```

```python
import functools

import jax
import jax.numpy as jnp
from jax import lax
from jax.experimental import pallas as pl
from jax.experimental.pallas import tpu as pltpu
from jax.sharding import PartitionSpec as P

ITERS = 4
PAD_GAIN = 8.0
SPECTRAL_BOUND = 0.995
G = ITERS
MESH = pl.DeviceIdType.MESH


def polynomial():
    weights = [1.0]
    for k in range(1, ITERS):
        if k == 1:
            weights.append(1.0 / (1.0 - SPECTRAL_BOUND**2 / 2.0))
        else:
            weights.append(1.0 / (1.0 - SPECTRAL_BOUND**2 * weights[-1] / 4.0))
    size = ITERS + 1
    previous = [1.0] + [0.0] * (size - 1)
    field = [1.0, 1.0] + [0.0] * (size - 2)
    for k in range(1, ITERS):
        jac = [1.0] + field[:-1]
        updated = [weights[k] * (a - b) + b for a, b in zip(jac, previous)]
        previous, field = field, updated
    return field


def loop(lo, count, width, compute):
    def turn(start, size):
        pending = [compute(start + u) for u in range(size)]
        for stores in pending:
            for put in stores:
                put()

    turns, rest = count // width, count % width
    if turns:
        lax.fori_loop(0, turns, lambda t, c: (turn(lo + t * width, width), c)[1], 0)
    if rest:
        turn(lo + turns * width, rest)


def setter(ref, index, value):
    def put():
        ref[index] = value
    return put


EAST, SOUTH, ROOT, FLAG = range(4)


def kernel(
    nx, ny, rows, cols,
    table_hbm, east_hbm, south_hbm, leak_hbm, pad_hbm, x_ref, o_ref,
    table_ref, east_ref, south_ref, leak_ref, pad_ref,
    cf, tw, passing, rim, pk, pe, load, src, v1, v2, v3, bc, eload,
    small_sem, rim_sem, local_sem, send_sem, recv_sem,
):
    mx, my = lax.axis_index("gx"), lax.axis_index("gy")
    north, south = lax.rem(mx + nx - 1, nx), lax.rem(mx + 1, nx)
    west, east = lax.rem(my + ny - 1, ny), lax.rem(my + 1, ny)
    cases = x_ref.shape[2]
    halves = [slice(h * 128, (h + 1) * 128) for h in range(cases // 128)]
    poly = polynomial()

    def settle(view, semaphore):
        pltpu.make_async_copy(view, view, semaphore).wait()

    barrier = pltpu.get_barrier_semaphore()
    peers = [(north, my), (south, my), (mx, west), (mx, east)]
    for peer in peers:
        pl.semaphore_signal(barrier, inc=1, device_id=peer, device_id_type=MESH)
    small = [
        pltpu.make_async_copy(there, here, small_sem.at[n])
        for n, (there, here) in enumerate([
            (table_hbm, table_ref), (east_hbm, east_ref), (south_hbm, south_ref),
            (leak_hbm, leak_ref), (pad_hbm, pad_ref),
        ])
    ]
    for copy in small:
        copy.start()
    area = pl.ds(G, rows)
    rims = [
        pltpu.make_async_copy(x_ref.at[:, pl.ds(0, G)], eload.at[0, area, pl.ds(G, G)], rim_sem),
        pltpu.make_async_copy(x_ref.at[:, pl.ds(cols - G, G)], eload.at[1, area, pl.ds(0, G)], rim_sem),
    ]
    for copy in rims:
        copy.start()
    borders = [
        pltpu.make_async_copy(x_ref.at[pl.ds(at, G)], load.at[pl.ds(at + G, G)], rim_sem)
        for at in [0, rows - G]
    ]
    rims += borders
    for copy in borders:
        copy.start()
    own = pltpu.make_async_copy(x_ref.at[pl.ds(G, rows - 2 * G)], load.at[pl.ds(2 * G, rows - 2 * G)], local_sem)
    own.start()
    for copy in small:
        copy.wait()

    def lookup(classes):
        value = jnp.full(classes.shape, table_ref[0], jnp.float32)
        for c in range(1, table_ref.shape[0]):
            value = jnp.where(classes == c, table_ref[c], value)
        return value

    blank = jnp.zeros((rows, 128 - cols), jnp.float32)
    fields = [
        lookup(east_ref[...]),
        lookup(south_ref[...]),
        leak_ref[...] + PAD_GAIN * pad_ref[...].astype(jnp.float32),
    ]
    for f in range(3):
        cf[f, pl.ds(8, rows), :] = jnp.concatenate([fields[f], blank], axis=1)

    lane = lax.broadcasted_iota(jnp.int32, (8, 128), 1)

    def transposed(f):
        return jnp.transpose(cf[f])[0:cols, :]

    def dense(lo, size):
        area = pl.ds(lo, size)
        e, s, extra = (cf[f, area, :] for f in range(3))
        root = lax.rsqrt(e + pltpu.roll(e, 1, 1) + s + pltpu.roll(s, 1, 0) + extra)
        flagged = jnp.where(extra > PAD_GAIN / 2, -root, root)
        left = jnp.broadcast_to(lane[0:1] < cols, (size, 128))
        after = pltpu.roll(root, size - 1, 0)
        values = [e * root * pltpu.roll(root, 127, 1), s * root * after, flagged, pltpu.roll(flagged, size - 1, 0)]
        for p in range(2):
            pk[p, area, :] = jnp.where(left, values[2 * p], pltpu.roll(values[2 * p + 1], cols, 1))

    def dense_edge(w, corners):
        values = []
        wide = jnp.broadcast_to(lane[0:1], (8, 128))
        for f in range(3):
            ghost = tw[f, pl.ds(w * (cols + 8), 8), :]
            if corners:
                ghost = jnp.where(wide < 8, pltpu.roll(passing[0, f, pl.ds(8 * w, 8), :], 128 - rows, 1), ghost)
                ghost = jnp.where(wide < rows + 8, ghost, pltpu.roll(passing[1, f, pl.ds(8 * w, 8), :], rows, 1))
            own_side = rim[f, pl.ds(16 * w, 16), :]
            values.append(jnp.concatenate([own_side, ghost] if w else [ghost, own_side], axis=0))
        e, s, extra = values
        root = lax.rsqrt(e + pltpu.roll(e, 1, 0) + s + pltpu.roll(s, 1, 1) + extra)
        flagged = jnp.where(extra > PAD_GAIN / 2, -root, root)
        values = [e * root * pltpu.roll(root, 23, 0), s * root * pltpu.roll(root, 127, 1), flagged]
        first = 16 - G if w else 8 - G
        return [value[first : first + 2 * G] for value in values]

    def turned(ref, r):
        return jnp.transpose(jnp.broadcast_to(ref[pl.ds(r + 8 - G, 1), :], (128, 128)))

    def scaled(flagged, value):
        return jnp.abs(flagged) * (jnp.where(flagged < 0.0, PAD_GAIN, 0.0) - value)

    def spread_rows(lo, count, loaded=True):
        inside = pl.ds(8, cols)
        stores = []
        for r in (lo + u for u in range(0, count, 2)):
            for v in range(2):
                value = turned(pk.at[0], r + v)
                stores.append(setter(bc, (EAST, r + v, inside), value[0:cols]))
                stores.append(setter(bc, (SOUTH, r + v, inside), value[cols : 2 * cols]))
            both = turned(pk.at[1], r)
            for v in range(2):
                value = both[v * cols : (v + 1) * cols]
                stores.append(setter(bc, (ROOT, r + v, inside), jnp.abs(value) * poly[ITERS]))
                if not loaded:
                    stores.append(setter(bc, (FLAG, r + v, inside), value))
                    continue
                for n, h in enumerate(halves):
                    stores.append(setter(src, (r + v, n, inside), scaled(value, load[r + v, :, h])))
        return stores

    def spread_edge(lo, count, width):
        def block(t):
            for u in range(0, width, 2):
                r = lo + t * width + u
                value = turned(pe, r)
                for v in range(2):
                    for w, at in enumerate([8 - G, 8 + cols - G]):
                        area = pl.ds(at, 2 * G)
                        e, s, flagged = (value[64 * v + 8 * (3 * w + f) :][: 2 * G] for f in range(3))
                        bc[EAST, r + v, area] = e
                        bc[SOUTH, r + v, area] = s
                        bc[FLAG, r + v, area] = flagged
                        bc[ROOT, r + v, area] = jnp.abs(flagged) * poly[ITERS]
        lax.fori_loop(0, count // width, lambda t, c: (block(t), c)[1], 0)

    above, below = jnp.zeros((8, 128), jnp.float32), jnp.zeros((120 - rows, 128), jnp.float32)
    for f in range(3):
        square = jnp.concatenate([above, jnp.concatenate([fields[f], blank], axis=1), below], axis=0)
        tw[f, pl.ds(8, cols), :] = jnp.transpose(square)[0:cols, :]
    dense(8, rows)
    early = 16
    for put in spread_rows(G, early, False):
        put()

    pl.semaphore_wait(barrier, len(peers))
    settle(load.at[pl.ds(0, 4 * G)], rim_sem)

    def send(source, target, device, group, bulk=1):
        copy = pltpu.make_async_remote_copy(
            src_ref=source, dst_ref=target,
            send_sem=send_sem.at[bulk], recv_sem=recv_sem.at[group],
            device_id=device, device_id_type=MESH,
        )
        copy.start()

    def eastward(at, count, group):
        part = pl.ds(at, count), pl.ds(0, G)
        send(eload.at[(1, *part)], eload.at[(0, *part)], (mx, east), group)

    def westward(at, count, group):
        part = pl.ds(at, count), pl.ds(G, G)
        send(eload.at[(0, *part)], eload.at[(1, *part)], (mx, west), group)

    cuts = [G + rows * part // 8 for part in (2, 4, 5, 6, 7)] + [rows]
    heads = [2 * G] + cuts[:-1]
    spans = [(lo, hi - lo) for lo, hi in zip(heads, cuts)]
    send(tw.at[:, pl.ds(cols + 2, 6)], tw.at[:, pl.ds(2, 6)], (mx, east), 0, 0)
    send(tw.at[:, pl.ds(8, G)], tw.at[:, pl.ds(cols + 8, G)], (mx, west), 0, 0)
    for way in (eastward, westward):
        way(G, G, 1)
        way(rows, G, 1)
    for way in (eastward, westward):
        for n, span in enumerate(spans):
            way(*span, 5 + n)
    send(cf.at[:, pl.ds(rows, 8)], cf.at[:, pl.ds(0, 8)], (south, my), 2, 0)
    send(cf.at[:, pl.ds(8, 8)], cf.at[:, pl.ds(rows + 8, 8)], (north, my), 2, 0)
    send(load.at[pl.ds(rows, G)], load.at[pl.ds(0, G)], (south, my), 3)
    send(load.at[pl.ds(G, G)], load.at[pl.ds(rows + G, G)], (north, my), 3)

    chain = [src, v1, v2, v3]

    def gather(r, at, size):
        coefs = [
            bc[EAST, r, pl.ds(at, size)], bc[EAST, r, pl.ds(at - 1, size)],
            bc[SOUTH, r, pl.ds(at, size)], bc[SOUTH, r - 1, pl.ds(at, size)],
        ]
        return coefs

    def update(k, r, n, at, size, coefs):
        vin = chain[k - 1]
        total = coefs[0] * vin[r, n, pl.ds(at + 1, size)]
        total += coefs[1] * vin[r, n, pl.ds(at - 1, size)]
        total += coefs[2] * vin[r + 1, n, pl.ds(at, size)]
        total += coefs[3] * vin[r - 1, n, pl.ds(at, size)]
        total = total + poly[ITERS - k] / poly[ITERS] * src[r, n, pl.ds(at, size)]
        if k == ITERS:
            total = total * bc[ROOT, r, pl.ds(at, size)]
        return total

    def step_row(k, r):
        skip = 2 * G if k == ITERS else G
        at, size = 8 + skip, cols - 2 * skip
        stores = []
        coefs = gather(r, at, size)
        for n, h in enumerate(halves):
            total = update(k, r, n, at, size, coefs)
            if k == ITERS:
                stores.append(setter(o_ref, (r - G, pl.ds(skip, size), h), total))
            else:
                stores.append(setter(chain[k], (r, n, pl.ds(at, size)), total))
        return stores

    def step(k, lo, count):
        loop(lo, count, 2, functools.partial(step_row, k))

    own.wait()

    def source_row(r):
        inside = pl.ds(8, cols)
        flagged = bc[FLAG, r, inside]
        return [setter(src, (r, n, inside), scaled(flagged, load[r, :, h])) for n, h in enumerate(halves)]

    loop(G, early, 2, source_row)
    W = 8

    def both(t):
        r = G + early + t * W
        stores = []
        for u in range(W):
            stores += step_row(1, r - W - 1 + u)
        stores += spread_rows(r, W)
        for put in stores:
            put()

    if early > W:
        step(1, G + 2, early - W - 3)
    turns = (rows - early) // W
    lax.fori_loop(0, turns, lambda t, c: (both(t), c)[1], 0)
    step(1, rows + G - W - 1, W)
    for k in range(2, ITERS + 1):
        step(k, G + k + 1, rows - 2 * k - 1)
        if k == 3:
            settle(cf.at[:, pl.ds(0, 6 + G)], recv_sem.at[0])
            for n, peer in enumerate([south, north]):
                for w, at in enumerate([0, cols + 8]):
                    send(tw.at[:, pl.ds(at, 8)], passing.at[n, :, pl.ds(8 * w, 8)], (peer, my), 4, 0)
            settle(eload.at[0, pl.ds(0, 2 * G)], recv_sem.at[1])
            for w in range(2):
                send(eload.at[w, pl.ds(rows, G)], eload.at[w, pl.ds(0, G)], (south, my), 5)
                send(eload.at[w, pl.ds(G, G)], eload.at[w, pl.ds(rows + G, G)], (north, my), 5)

    settle(cf.at[:, pl.ds(0, 16)], recv_sem.at[2])
    dense(0, rows + 16)
    for put in spread_rows(0, G + 2, False) + spread_rows(rows + G - 2, G + 2, False):
        put()

    def edge_fields(corners):
        stack = jnp.concatenate(dense_edge(0, corners) + dense_edge(1, corners) + [jnp.zeros((16, 128), jnp.float32)], axis=0)
        pe[...] = jnp.transpose(jnp.concatenate([stack, pltpu.roll(stack, 127, 1)], axis=0))

    for f in range(3):
        whole = transposed(f)
        rim[f] = jnp.concatenate([whole[0:16], whole[cols - 16 :]], axis=0)
    edge_fields(False)
    spread_edge(2 * G, rows - 2 * G, 28)

    settle(load.at[pl.ds(0, 2 * G)], recv_sem.at[3])
    loop(0, G + 1, 2, source_row)
    loop(rows + G, G, 2, source_row)
    for k in range(1, ITERS + 1):
        step(k, k, G + 1)
        step(k, rows + 2 * G - k - G, G)
    settle(cf.at[:, pl.ds(0, 32)], recv_sem.at[4])
    edge_fields(True)
    spread_edge(0, 2 * G, 2 * G)
    spread_edge(rows, 2 * G, 2 * G)

    edge = 2 * G
    rims_at = [[8 - G, 9 - G, 9 - G, 10 - G, 8], [8 + cols - G, 7 + cols - G, 7 + cols - G, 6 + cols - G, 8 + cols - 2 * G]]

    def edge_source(lo, count):
        def one(r):
            stores = []
            for w in range(2):
                area = pl.ds(rims_at[w][0], edge)
                flagged = bc[FLAG, r, area]
                for n, h in enumerate(halves):
                    stores.append(setter(src, (r, n, area), scaled(flagged, eload[w, r, :, h])))
            return stores
        loop(lo, count, 4, one)

    def edge_step(k, lo, count):
        def one(r):
            stores = []
            for w in range(2):
                at = rims_at[w][k]
                coefs = gather(r, at, edge)
                for n, h in enumerate(halves):
                    total = update(k, r, n, at, edge, coefs)
                    if k < ITERS:
                        stores.append(setter(chain[k], (r, n, pl.ds(at, edge)), total))
                    else:
                        stores.append(setter(o_ref, (r - G, pl.ds(at - 8, edge), h), total))
            return stores

        loop(lo, count, 4, one)

    bounds = [0] + cuts
    for m, (_, count) in enumerate(spans):
        settle(eload.at[0, pl.ds(0, count if m else count + 4 * G)], recv_sem.at[5 + m])
        lo, hi = bounds[m], bounds[m + 1]
        last = m == len(spans) - 1
        edge_source(lo, hi - lo)
        for k in range(1, ITERS + 1):
            begin = k if m == 0 else lo - k
            edge_step(k, begin, (hi + k if last else hi - k) - begin)
        if m == 0:
            edge_source(rows, 2 * G)
            for k in range(1, G):
                edge_step(k, rows + k, 2 * G - 2 * k)
    settle(cf.at[:, pl.ds(0, 6 + G + 16 + 32)], send_sem.at[0])
    sent = 2 * rows * G + 2 * G * cols + 4 * G * 2 * G
    settle(load.at[pl.ds(0, sent // cols)], send_sem.at[1])


def body(nx, ny, east_class, south_class, cond_table, leakage, pad_mask, load_current):
    rows, cols, cases = load_current.shape
    tall = rows + 2 * G
    f32 = jnp.float32
    halves = cases // 128
    anywhere = pl.BlockSpec(memory_space=pl.ANY)
    grid = (tall, halves, cols + 16, 128)
    return pl.pallas_call(
        functools.partial(kernel, nx, ny, rows, cols),
        out_shape=pltpu.VMEM(load_current.shape, f32),
        in_specs=[anywhere] * 6,
        out_specs=pl.BlockSpec(memory_space=pltpu.VMEM),
        scratch_shapes=[
            pltpu.SMEM(cond_table.shape, f32),
            pltpu.VMEM((rows, cols), jnp.int32),
            pltpu.VMEM((rows, cols), jnp.int32),
            pltpu.VMEM((rows, cols), f32),
            pltpu.VMEM((rows, cols), jnp.int32),
            pltpu.VMEM((3, 128, 128), f32),
            pltpu.VMEM((3, cols + 16, 128), f32),
            pltpu.VMEM((2, 3, 16, 128), f32),
            pltpu.VMEM((3, 32, 128), f32),
            pltpu.VMEM((2, 128, 128), f32),
            pltpu.VMEM((128, 128), f32),
            pltpu.VMEM((tall, cols, cases), f32),
            pltpu.VMEM(grid, f32),
            pltpu.VMEM(grid, f32),
            pltpu.VMEM(grid, f32),
            pltpu.VMEM(grid, f32),
            pltpu.VMEM((4, tall, cols + 16, 128), f32),
            pltpu.VMEM((2, tall, 2 * G, cases), f32),
            pltpu.SemaphoreType.DMA((5,)),
            pltpu.SemaphoreType.DMA,
            pltpu.SemaphoreType.DMA,
            pltpu.SemaphoreType.DMA((2,)),
            pltpu.SemaphoreType.DMA((11,)),
        ],
        compiler_params=pltpu.CompilerParams(
            collective_id=0, has_side_effects=True, vmem_limit_bytes=57 * 2**20,
        ),
    )(cond_table, east_class, south_class, leakage, pad_mask, load_current)


def solution(mesh):
    in_specs = (
        P("gx", "gy"),
        P("gx", "gy"),
        P(),
        P("gx", "gy"),
        P("gx", "gy"),
        P("gx", "gy", None),
    )
    out_specs = P("gx", "gy", None)
    call = functools.partial(body, mesh.shape["gx"], mesh.shape["gy"])
    return jax.shard_map(call, mesh=mesh, in_specs=in_specs, out_specs=out_specs, check_vma=False)
```
